512 devices in a mesh: cell: 64 (over x, z, core), grp: 8 (over y).
Axes of the slice: x: 4, y: 8, z: 8, core: 2. Of those that a mesh axis runs over, the one named last changes fastest.
Arguments:
- atom_sites: float32 [3, 262144], P(None, ('cell', 'grp')), may hold values from 0 to 64, as said below
- grid_points: float32 [3, 196608], P(None, ('cell', 'grp')), may hold values from 0 to 64, as said below
- dipole_guess: float32 [3, 262144], P(None, ('cell', 'grp')), may hold values from -2 to 2
- fixed_field: float32 [3, 262144], P(None, ('cell', 'grp')), may hold values from -1800 to 1800
- polarisability: float32 [262144], P(('cell', 'grp')), may hold values from 0.0005 to 0.002
- base_charge: float32 [196608], P(('cell', 'grp')), may hold values from -12 to 12
- response: float32 [196608], P(('cell', 'grp')), may hold values from 0.02 to 0.2
- near_blocks: int32 [2048, 8], P(('cell', 'grp')), may hold values from 0 to 95, as said below
- grid_blocks: int32 [2048, 4], P(('cell', 'grp')), may hold values from 0 to 71, as said below
- source_blocks: int32 [1536, 8], P(('cell', 'grp')), may hold values from 0 to 95, as said below
Outputs:
- dipoles: float32 [3, 262144], P(None, ('cell', 'grp'))
- qm_charges: float32 [196608], P(('cell', 'grp'))
The draws below stay inside these ranges and needn't reach their ends.
Inputs may be any that keep to these rules, and one draw needn't show every extreme that they name: `atom_sites`: atom a has first coordinate in [c, c + 1) with c = a // 4096, the other two in [0, 1). `grid_points`: grid point g has first coordinate in [c, c + 1) with c = g // 3072, the other two in [0, 1). `near_blocks`: each row holds 8 distinct MM window indices, never the block's own index 32 + b % 32. `grid_blocks`: each row holds 4 distinct grid window indices. `source_blocks`: each row holds 8 distinct MM window indices.
All inputs are finite; a program needn't handle non-finite values.
Results may differ from the reference program's by a relative error of at most 0.0003.
Values sent between devices are 32-bit elements; how exact they have to be, the bound alone decides.
A program may use at most 64 MiB of HBM per device.

```python
import math
import jax
import jax.numpy as jnp
from jax import lax

BLOCK = 128
NB = 8
NQ = 4
NM = 8
ITERS = 3
CELLS = 64
CELL_BLK = 32
CELL_GBLK = 24
CELL_ATOMS = 4096
CELL_GRID = 3072
BLOCKS = 2048
GBLOCKS = 1536
ATOMS = 262144
GRID = 196608


def place_points(key, per_cell):
    uniform_unit = jax.random.uniform(key, (3, CELLS * per_cell), jnp.float32)
    shift_x = (jnp.arange(CELLS * per_cell, dtype=jnp.int32) // per_cell).astype(jnp.float32)
    return jnp.stack([uniform_unit[0] + shift_x, uniform_unit[1], uniform_unit[2]])


def window_lists(key, row_count, span, picks, cell_rows, exclude_own):
    scores = jax.random.randint(key, (row_count, span), 0, 1 << 20, dtype=jnp.int32) * span
    scores = scores + jnp.arange(span, dtype=jnp.int32)[None, :]
    if exclude_own:
        own_rows = cell_rows + jnp.arange(row_count, dtype=jnp.int32) % cell_rows
        scores = jnp.where(jnp.arange(span, dtype=jnp.int32)[None, :] == own_rows[:, None], -1, scores)
    return lax.top_k(scores, picks)[1].astype(jnp.int32)


def draw_atom_sites(key, part):
    return place_points(jax.random.fold_in(key, 11), CELL_ATOMS)


def draw_grid_points(key, part):
    return place_points(jax.random.fold_in(key, 12), CELL_GRID)


def draw_near_blocks(key, part):
    return window_lists(jax.random.fold_in(key, 21), BLOCKS, 3 * CELL_BLK, NB, CELL_BLK, True)


def draw_grid_blocks(key, part):
    return window_lists(jax.random.fold_in(key, 22), BLOCKS, 3 * CELL_GBLK, NQ, CELL_GBLK, False)


def draw_source_blocks(key, part):
    return window_lists(jax.random.fold_in(key, 23), GBLOCKS, 3 * CELL_BLK, NM, CELL_BLK, False)


def level_of(own_key, dims, shards, low, top_value):
    def one(dim, blocks):
        steps = jax.random.uniform(jax.random.fold_in(jax.random.fold_in(own_key, 6), dim), (blocks,), jnp.float32, low / len(shards), top_value / len(shards))
        return jnp.repeat(jnp.exp(steps), dims[dim] // blocks).reshape((-1,) + (1,) * (len(dims) - dim - 1))

    gain = one(*shards[0])
    for cut in shards[1:]:
        gain = gain * one(*cut)
    return gain


def scatter_about(own_key, extent, deviation, bound, shards=(), kind=jnp.bfloat16):
    gain = level_of(own_key, extent, shards, -0.22, 0.18) if shards else 1.0
    values = jax.random.normal(own_key, extent, jnp.float32) * deviation * gain
    return jnp.minimum(jnp.maximum(values, -bound), bound).astype(kind)


def setup_inputs(seed: int = 0) -> dict:
    arg_keys = jax.random.split(jax.random.key(seed), 11)
    atom_sites = draw_atom_sites(jax.random.fold_in(arg_keys[10], 71), 0)
    grid_points = draw_grid_points(jax.random.fold_in(arg_keys[10], 71), 0)
    dipole_guess = scatter_about(arg_keys[2], (3, ATOMS), 0.3, 2.0, ((1, 512),), jnp.float32)
    fixed_field = scatter_about(arg_keys[3], (3, ATOMS), 300.0, 1800.0, ((1, 512),), jnp.float32)
    polarisability = jnp.clip(jnp.exp(math.log(0.002) - 1.3862944 * jax.random.uniform(arg_keys[4], (ATOMS,), jnp.float32) ** level_of(arg_keys[4], (ATOMS,), ((0, 512),), -0.2, 0.2)), 0.0005, 0.002)
    base_charge = scatter_about(arg_keys[5], (GRID,), 2.0, 12.0, ((0, 512),), jnp.float32)
    response = jnp.clip(jnp.exp(math.log(0.2) - 2.3025851 * jax.random.uniform(arg_keys[6], (GRID,), jnp.float32) ** level_of(arg_keys[6], (GRID,), ((0, 512),), -0.2, 0.2)), 0.02, 0.2)
    near_blocks = draw_near_blocks(jax.random.fold_in(arg_keys[10], 71), 0)
    grid_blocks = draw_grid_blocks(jax.random.fold_in(arg_keys[10], 71), 0)
    source_blocks = draw_source_blocks(jax.random.fold_in(arg_keys[10], 71), 0)
    return dict(atom_sites=atom_sites, grid_points=grid_points, dipole_guess=dipole_guess, fixed_field=fixed_field, polarisability=polarisability, base_charge=base_charge, response=response, near_blocks=near_blocks, grid_blocks=grid_blocks, source_blocks=source_blocks)


soften_sq = 0.04

def pick_tile(tile_set, slot_index):
    return lax.dynamic_index_in_dim(tile_set, slot_index, 1, keepdims=False)

def pair_geometry(targets, sources):
    delta_x = targets[0][:, None] - sources[0][None, :]
    delta_y = targets[1][:, None] - sources[1][None, :]
    delta_z = targets[2][:, None] - sources[2][None, :]
    inverse = 1.0 / jnp.sqrt(delta_x * delta_x + delta_y * delta_y + delta_z * delta_z + soften_sq)
    inv_cube = inverse * inverse * inverse
    return (delta_x, delta_y, delta_z, inv_cube, inv_cube * inverse * inverse)

def dipole_field(targets, sources, moments, keep_mask):
    delta_x, delta_y, delta_z, inv_cube, inv_fifth = pair_geometry(targets, sources)
    projected = moments[0][None, :] * delta_x + moments[1][None, :] * delta_y + moments[2][None, :] * delta_z
    radial = 3.0 * projected * inv_fifth * keep_mask
    direct = inv_cube * keep_mask
    return jnp.stack([lax.optimization_barrier(jnp.sum(radial * delta_x - moments[0][None, :] * direct, axis=1)), lax.optimization_barrier(jnp.sum(radial * delta_y - moments[1][None, :] * direct, axis=1)), lax.optimization_barrier(jnp.sum(radial * delta_z - moments[2][None, :] * direct, axis=1))])

def charge_field(targets, sources, charges):
    delta_x, delta_y, delta_z, inv_cube, inv_fifth = pair_geometry(targets, sources)
    weight = charges[None, :] * inv_cube
    return jnp.stack([lax.optimization_barrier(jnp.sum(weight * delta_x, axis=1)), lax.optimization_barrier(jnp.sum(weight * delta_y, axis=1)), lax.optimization_barrier(jnp.sum(weight * delta_z, axis=1))])

def dipole_potential(targets, sources, moments):
    delta_x, delta_y, delta_z, inv_cube, inv_fifth = pair_geometry(targets, sources)
    projected = moments[0][None, :] * delta_x + moments[1][None, :] * delta_y + moments[2][None, :] * delta_z
    return lax.optimization_barrier(jnp.sum(projected * inv_cube, axis=1))

def far_geometry(targets, cell_here, cell_count):
    centres = jnp.arange(cell_count, dtype=jnp.int32).astype(jnp.float32) + 0.5
    delta_x = targets[0][None, :] - centres[:, None]
    delta_y = targets[1][None, :] - 0.5
    delta_z = targets[2][None, :] - 0.5
    far_mask = (jnp.abs(jnp.arange(cell_count, dtype=jnp.int32) - cell_here) >= 2).astype(jnp.float32)[:, None]
    inverse = 1.0 / jnp.sqrt(delta_x * delta_x + delta_y * delta_y + delta_z * delta_z + soften_sq)
    inv_cube = inverse * inverse * inverse * far_mask
    return (delta_x, delta_y, delta_z, inv_cube, inv_cube * inverse * inverse)

def far_field(targets, cell_here, moments, charges):
    delta_x, delta_y, delta_z, inv_cube, inv_fifth = far_geometry(targets, cell_here, charges.shape[0])
    projected = moments[:, 0:1] * delta_x + moments[:, 1:2] * delta_y + moments[:, 2:3] * delta_z
    radial = 3.0 * projected * inv_fifth
    coulomb = charges[:, None] * inv_cube
    return jnp.stack([lax.optimization_barrier(jnp.sum(radial * delta_x - moments[:, 0:1] * inv_cube + coulomb * delta_x, axis=0)), lax.optimization_barrier(jnp.sum(radial * delta_y - moments[:, 1:2] * inv_cube + coulomb * delta_y, axis=0)), lax.optimization_barrier(jnp.sum(radial * delta_z - moments[:, 2:3] * inv_cube + coulomb * delta_z, axis=0))])

def far_potential(targets, cell_here, moments):
    delta_x, delta_y, delta_z, inv_cube, inv_fifth = far_geometry(targets, cell_here, moments.shape[0])
    projected = moments[:, 0:1] * delta_x + moments[:, 1:2] * delta_y + moments[:, 2:3] * delta_z
    return lax.optimization_barrier(jnp.sum(projected * inv_cube, axis=0))

def atom_block(targets, own_slot, near_list, grid_list, site_tiles, dipole_tiles, point_tiles, charge_tiles, cell_here, moments, charge_sums):
    tile_width = targets.shape[1]
    self_mask = 1.0 - jnp.eye(tile_width, dtype=jnp.float32)
    accumulated = dipole_field(targets, pick_tile(site_tiles, own_slot), pick_tile(dipole_tiles, own_slot), self_mask)

    def near_step(member, carried):
        other_slot = near_list[member]
        return carried + dipole_field(targets, pick_tile(site_tiles, other_slot), pick_tile(dipole_tiles, other_slot), 1.0)
    accumulated = lax.fori_loop(0, near_list.shape[0], near_step, accumulated)

    def grid_step(member, carried):
        other_slot = grid_list[member]
        return carried + charge_field(targets, pick_tile(point_tiles, other_slot), lax.dynamic_index_in_dim(charge_tiles, other_slot, 0, keepdims=False))
    accumulated = lax.fori_loop(0, grid_list.shape[0], grid_step, accumulated)
    return accumulated + far_field(targets, cell_here, moments, charge_sums)

def grid_block(targets, source_list, site_tiles, dipole_tiles, cell_here, dipole_sums):

    def near_step(member, carried):
        other_slot = source_list[member]
        return carried + dipole_potential(targets, pick_tile(site_tiles, other_slot), pick_tile(dipole_tiles, other_slot))
    accumulated = lax.fori_loop(0, source_list.shape[0], near_step, jnp.zeros((targets.shape[1],), jnp.float32))
    return accumulated + far_potential(targets, cell_here, dipole_sums)

def cell_table(dipoles, charges, grid_points):
    dipole_sums = lax.optimization_barrier(jnp.sum(dipoles.reshape(3, CELLS, CELL_ATOMS), axis=2)).T
    charge_cells = charges.reshape(CELLS, CELL_GRID)
    centres = jnp.stack([jnp.arange(CELLS, dtype=jnp.int32).astype(jnp.float32) + 0.5, jnp.full((CELLS,), 0.5, jnp.float32), jnp.full((CELLS,), 0.5, jnp.float32)])
    offsets = grid_points.reshape(3, CELLS, CELL_GRID) - centres[:, :, None]
    charge_sums = lax.optimization_barrier(jnp.sum(charge_cells, axis=1))
    grid_moments = lax.optimization_barrier(jnp.sum(charge_cells[None, :, :] * offsets, axis=2)).T
    return (dipole_sums, charge_sums, grid_moments)

def reference(atom_sites, grid_points, dipole_guess, fixed_field, polarisability, base_charge, response, near_blocks, grid_blocks, source_blocks):
    target_tiles = atom_sites.reshape(3, BLOCKS, BLOCK)
    grid_targets = grid_points.reshape(3, GBLOCKS, BLOCK)
    site_tiles = jnp.pad(target_tiles, ((0, 0), (CELL_BLK, CELL_BLK), (0, 0)))
    point_tiles = jnp.pad(grid_targets, ((0, 0), (CELL_GBLK, CELL_GBLK), (0, 0)))
    dipoles = dipole_guess
    charges = base_charge
    for iteration in range(ITERS):
        dipole_sums, charge_sums, grid_moments = cell_table(dipoles, charges, grid_points)
        moments = dipole_sums + grid_moments
        dipole_tiles = jnp.pad(dipoles.reshape(3, BLOCKS, BLOCK), ((0, 0), (CELL_BLK, CELL_BLK), (0, 0)))
        charge_tiles = jnp.pad(charges.reshape(GBLOCKS, BLOCK), ((CELL_GBLK, CELL_GBLK), (0, 0)))

        def one_atom_block(block_index):
            cell_here = block_index // CELL_BLK
            window_start = cell_here * CELL_BLK
            grid_start = cell_here * CELL_GBLK
            return atom_block(pick_tile(target_tiles, block_index), block_index - window_start + CELL_BLK, near_blocks[block_index], grid_blocks[block_index], lax.dynamic_slice_in_dim(site_tiles, window_start, 3 * CELL_BLK, 1), lax.dynamic_slice_in_dim(dipole_tiles, window_start, 3 * CELL_BLK, 1), lax.dynamic_slice_in_dim(point_tiles, grid_start, 3 * CELL_GBLK, 1), lax.dynamic_slice_in_dim(charge_tiles, grid_start, 3 * CELL_GBLK, 0), cell_here, moments, charge_sums)

        def one_grid_block(block_index):
            cell_here = block_index // CELL_GBLK
            window_start = cell_here * CELL_BLK
            return grid_block(pick_tile(grid_targets, block_index), source_blocks[block_index], lax.dynamic_slice_in_dim(site_tiles, window_start, 3 * CELL_BLK, 1), lax.dynamic_slice_in_dim(dipole_tiles, window_start, 3 * CELL_BLK, 1), cell_here, dipole_sums)
        induced_field = lax.map(one_atom_block, jnp.arange(BLOCKS, dtype=jnp.int32))
        induced_field = jnp.transpose(induced_field, (1, 0, 2)).reshape(3, ATOMS)
        potential = lax.map(one_grid_block, jnp.arange(GBLOCKS, dtype=jnp.int32)).reshape(GRID)
        dipoles = polarisability[None, :] * (fixed_field + induced_field)
        charges = base_charge - response * potential
    return (dipoles, charges)
```

```python
import functools

import jax
import jax.numpy as jnp
from jax import lax
from jax.experimental import pallas as pl
from jax.experimental.pallas import tpu as pltpu
from jax.sharding import PartitionSpec as P

BLOCK = 128
ITERS = 3
CHUNK = 32
SOFT = 0.04
MESH = pl.DeviceIdType.MESH
F32 = jnp.float32


def copy_to(src, dst, send_sem, recv_sem, device):
    pltpu.make_async_remote_copy(
        src_ref=src,
        dst_ref=dst,
        send_sem=send_sem,
        recv_sem=recv_sem,
        device_id=device,
        device_id_type=MESH,
    ).start()


def drain(ref, sem):
    pltpu.make_async_copy(ref, ref, sem).wait()


def powers(dx, dy, dz):
    s = lax.rsqrt(dx * dx + dy * dy + dz * dz + SOFT)
    s2 = s * s
    s3 = s2 * s
    return s3, s3 * s2


def pair_tensor(dx, dy, dz, s3, s5):
    t = 3.0 * s5
    tx, ty, tz = t * dx, t * dy, t * dz
    return (tx * dx - s3, tx * dy, tx * dz, ty * dy - s3, ty * dz, tz * dz - s3)


def kernel(
    ncell, ngrp, lb, lg, nb, nq, nm,
    near_list, grid_list, source_list,
    sites, points, guess, fixed, pol, base, resp,
    out_mu, out_q,
    w0, w1, w2, pos, sa, tb0, tb1, tb2,
    tgt, td, tc, tp, fd, fp, fb, mub, mus, qub, accs, nf, gp,
    send_sem, recv_sem,
):
    windows = (w0, w1, w2)
    tables = (tb0, tb1, tb2)
    cell = lax.axis_index("cell")
    grp = lax.axis_index("grp")
    urows = 3 * lb + lg
    prows = 3 * lb + 3 * lg
    slots = nb + 1
    own = ngrp + grp

    barrier = pltpu.get_barrier_semaphore()

    def greet_far(d, carry):
        pl.semaphore_signal(
            barrier, inc=1, device_id=(lax.rem(cell + d, ncell), grp), device_id_type=MESH
        )
        return carry

    def greet_group(d, carry):
        pl.semaphore_signal(
            barrier, inc=1, device_id=(cell, lax.rem(grp + d, ngrp)), device_id_type=MESH
        )
        return carry

    lax.fori_loop(1, ncell, greet_far, 0)
    lax.fori_loop(1, ngrp, greet_group, 0)

    def lanes(j):
        return pl.ds(j * BLOCK, BLOCK)

    zc = [cell.astype(F32) + 0.5, 0.5, 0.5]
    lane = lax.broadcasted_iota(jnp.int32, (1, BLOCK), 1)

    def put_state(k, mu, q):
        w = windows[k]
        for a in range(3):
            for b in range(lb):
                w[own * urows + a * lb + b] = mu[a][b]
        for g in range(lg):
            w[own * urows + 3 * lb + g] = q[g]
        sums = [functools.reduce(jnp.add, mu[a]) for a in range(3)]
        sums.append(functools.reduce(jnp.add, q))
        for a in range(3):
            moment = functools.reduce(
                jnp.add, [q[g] * (points[a : a + 1, lanes(g)] - zc[a]) for g in range(lg)]
            )
            sums.append(moment + sums[a])
        row = jnp.zeros((1, BLOCK), F32)
        for n, s in enumerate(sums):
            row = jnp.where(lane == n, jnp.sum(s, axis=1, keepdims=True), row)
        sa[k * ngrp + grp] = row

    for a in range(3):
        for b in range(lb):
            pos[own * prows + a * lb + b] = sites[a : a + 1, lanes(b)]
        for g in range(lg):
            pos[own * prows + 3 * lb + a * lg + g] = points[a : a + 1, lanes(g)]
    put_state(
        0,
        [[guess[a : a + 1, lanes(b)] for b in range(lb)] for a in range(3)],
        [base[0:1, lanes(g)] for g in range(lg)],
    )

    def clear(start):
        for w in windows:
            w[pl.ds(start * ngrp * urows, ngrp * urows)] = jnp.zeros(
                (ngrp * urows, 1, BLOCK), F32
            )
        pos[pl.ds(start * ngrp * prows, ngrp * prows)] = jnp.zeros((ngrp * prows, 1, BLOCK), F32)

    @pl.when(cell == 0)
    def _():
        clear(0)

    @pl.when(cell == ncell - 1)
    def _():
        clear(2)

    for a in range(3):
        for b in range(lb):
            tgt[b * 3 + a] = jnp.transpose(
                jnp.broadcast_to(sites[a : a + 1, lanes(b)], (BLOCK, BLOCK))
            )
        for g in range(lg):
            tgt[(lb + g) * 3 + a] = jnp.transpose(
                jnp.broadcast_to(points[a : a + 1, lanes(g)], (BLOCK, BLOCK))
            )

    cells8 = lax.broadcasted_iota(jnp.int32, (8, BLOCK), 0)

    def far_rows(ref, j, c8):
        number = cells8 + c8 * 8
        dx = ref[0:1, lanes(j)] - (number.astype(F32) + 0.5)
        dy = ref[1:2, lanes(j)] - 0.5 + jnp.zeros_like(dx)
        dz = ref[2:3, lanes(j)] - 0.5 + jnp.zeros_like(dx)
        keep = jnp.abs(number - cell) >= 2
        s3, s5 = powers(dx, dy, dz)
        return dx, dy, dz, jnp.where(keep, s3, 0.0), jnp.where(keep, s5, 0.0)

    def far_build(c8, carry):
        row = pl.ds(pl.multiple_of(c8 * 8, 8), 8)
        for b in range(lb):
            dx, dy, dz, s3, s5 = far_rows(sites, b, c8)
            for n, v in enumerate(pair_tensor(dx, dy, dz, s3, s5)):
                fd[b * 9 + n, row] = v
            for n, v in enumerate((dx, dy, dz)):
                fd[b * 9 + 6 + n, row] = v * s3
        for g in range(lg):
            dx, dy, dz, s3, s5 = far_rows(points, g, c8)
            for n, v in enumerate((dx, dy, dz)):
                fp[g * 3 + n, row] = v * s3
        return carry

    lax.fori_loop(0, ncell // 8, far_build, 0)

    pl.semaphore_wait(barrier, ncell + ngrp - 2)

    S_SA, S_W, S_FL, S_FR, S_TB = 0, 3, 6, 9, 12
    S_POS, S_PL, S_PR = 15, 16, 17

    def share_group(ref, start, count, sem):
        def step(d, carry):
            part = ref.at[pl.ds(start, count)]
            copy_to(
                part, part, send_sem.at[sem], recv_sem.at[sem], (cell, lax.rem(grp + d, ngrp))
            )
            return carry

        lax.fori_loop(1, ngrp, step, 0)

    def share_sums(k):
        share_group(sa, k * ngrp + grp, 1, S_SA + k)

    def share_state(k):
        share_group(windows[k], own * urows, urows, S_W + k)

    def share_cell(k):
        drain(sa.at[pl.ds(0, ngrp - 1)], recv_sem.at[S_SA + k])
        total = functools.reduce(jnp.add, [sa[k * ngrp + j] for j in range(ngrp)])
        table = tables[k]
        table[cell] = total

        def step(d, carry):
            part = table.at[pl.ds(cell, 1)]
            copy_to(
                part,
                part,
                send_sem.at[S_TB + k],
                recv_sem.at[S_TB + k],
                (lax.rem(cell + d, ncell), grp),
            )
            return carry

        lax.fori_loop(1, ncell, step, 0)

    def forward(ref, rows, sem_group, sem_left, sem_right):
        drain(ref.at[pl.ds(0, (ngrp - 1) * rows)], recv_sem.at[sem_group])
        size = ngrp * rows
        mine = ref.at[pl.ds(size, size)]

        @pl.when(cell < ncell - 1)
        def _():
            copy_to(
                mine, ref.at[pl.ds(0, size)],
                send_sem.at[sem_right], recv_sem.at[sem_right], (cell + 1, grp),
            )

        @pl.when(cell > 0)
        def _():
            copy_to(
                mine, ref.at[pl.ds(2 * size, size)],
                send_sem.at[sem_left], recv_sem.at[sem_left], (cell - 1, grp),
            )

    def arrived(ref, rows, sem_left, sem_right):
        size = ngrp * rows

        @pl.when(cell > 0)
        def _():
            drain(ref.at[pl.ds(0, size)], recv_sem.at[sem_right])

        @pl.when(cell < ncell - 1)
        def _():
            drain(ref.at[pl.ds(2 * size, size)], recv_sem.at[sem_left])

    def block_row(w, rows, offset):
        return (w // lb) * rows + lax.rem(w, lb) + offset

    def point_row(w, rows, offset):
        return (w // lg) * rows + lax.rem(w, lg) + offset

    def source_slot(b, s):
        return (ngrp + grp) * lb + b if s == 0 else near_list[b, s - 1]

    def build():
        diagonal = (
            lax.broadcasted_iota(jnp.int32, (CHUNK, BLOCK), 1)
            - lax.broadcasted_iota(jnp.int32, (CHUNK, BLOCK), 0)
        )

        def deltas(t, j, rows):
            row = pl.ds(pl.multiple_of(t * CHUNK, CHUNK), CHUNK)
            return row, [tgt[j * 3 + a, row] - rows[a] for a in range(3)]

        def atoms(b, carry):
            for s in range(slots):
                r = block_row(source_slot(b, s), prows, 0)
                rows = [pos[r + a * lb] for a in range(3)]

                def step(t, c, s=s, rows=rows):
                    row, (dx, dy, dz) = deltas(t, b, rows)
                    s3, s5 = powers(dx, dy, dz)
                    if s == 0:
                        s3 = jnp.where(diagonal == t * CHUNK, 0.0, s3)
                    for n, v in enumerate(pair_tensor(dx, dy, dz, s3, s5)):
                        td[(b * slots + s) * 6 + n, row] = v
                    return c

                lax.fori_loop(0, BLOCK // CHUNK, step, 0)
            for s in range(nq):
                r = point_row(grid_list[b, s], prows, 3 * lb)
                rows = [pos[r + a * lg] for a in range(3)]

                def step(t, c, s=s, rows=rows):
                    row, (dx, dy, dz) = deltas(t, b, rows)
                    s3, s5 = powers(dx, dy, dz)
                    for n, v in enumerate((dx, dy, dz)):
                        tc[(b * nq + s) * 3 + n, row] = v * s3
                    return c

                lax.fori_loop(0, BLOCK // CHUNK, step, 0)
            return carry

        lax.fori_loop(0, lb, atoms, 0)

        def grids(g, carry):
            for s in range(nm):
                r = block_row(source_list[g, s], prows, 0)
                rows = [pos[r + a * lb] for a in range(3)]

                def step(t, c, s=s, rows=rows):
                    row, (dx, dy, dz) = deltas(t, lb + g, rows)
                    s3, s5 = powers(dx, dy, dz)
                    for n, v in enumerate((dx, dy, dz)):
                        tp[(g * nm + s) * 3 + n, row] = v * s3
                    return c

                lax.fori_loop(0, BLOCK // CHUNK, step, 0)
            return carry

        lax.fori_loop(0, lg, grids, 0)

    def apply_near(w):
        def wide(row):
            return jnp.broadcast_to(row, (8, BLOCK))

        def pick_atoms(b, carry):
            for s in range(slots):
                r = block_row(source_slot(b, s), urows, 0)
                for a in range(3):
                    mub[(b * slots + s) * 3 + a] = wide(w[r + a * lb])
            for s in range(nq):
                qub[b * nq + s] = wide(w[point_row(grid_list[b, s], urows, 3 * lb)])
            return carry

        lax.fori_loop(0, lb, pick_atoms, 0)

        def pick_grids(g, carry):
            for s in range(nm):
                r = block_row(source_list[g, s], urows, 0)
                for a in range(3):
                    mus[(g * nm + s) * 3 + a] = wide(w[r + a * lb])
            return carry

        lax.fori_loop(0, lg, pick_grids, 0)

        parts = CHUNK // 8

        def atoms(j, carry):
            b = j // (BLOCK // CHUNK)
            start = lax.rem(j, BLOCK // CHUNK) * CHUNK
            rows = [pl.ds(pl.multiple_of(start + 8 * i, 8), 8) for i in range(parts)]
            acc = [[jnp.zeros((8, BLOCK), F32) for _ in range(parts)] for _ in range(3)]
            for s in range(slots):
                mx, my, mz = [mub[(b * slots + s) * 3 + a] for a in range(3)]
                at = (b * slots + s) * 6
                for i in range(parts):
                    xx, xy, xz, yy, yz, zz = [td[at + n, rows[i]] for n in range(6)]
                    acc[0][i] = acc[0][i] + (xx * mx + xy * my + xz * mz)
                    acc[1][i] = acc[1][i] + (xy * mx + yy * my + yz * mz)
                    acc[2][i] = acc[2][i] + (xz * mx + yz * my + zz * mz)
            for s in range(nq):
                q = qub[b * nq + s]
                for i in range(parts):
                    for a in range(3):
                        acc[a][i] = acc[a][i] + tc[(b * nq + s) * 3 + a, rows[i]] * q
            for a in range(3):
                for i in range(parts):
                    accs[b * 3 + a, rows[i]] = acc[a][i]
            return carry

        lax.fori_loop(0, lb * (BLOCK // CHUNK), atoms, 0)

        def grids(j, carry):
            g = j // (BLOCK // CHUNK)
            start = lax.rem(j, BLOCK // CHUNK) * CHUNK
            rows = [pl.ds(pl.multiple_of(start + 8 * i, 8), 8) for i in range(parts)]
            acc = [jnp.zeros((8, BLOCK), F32) for _ in range(parts)]
            for s in range(nm):
                m = [mus[(g * nm + s) * 3 + a] for a in range(3)]
                at = (g * nm + s) * 3
                for i in range(parts):
                    acc[i] = acc[i] + (
                        tp[at, rows[i]] * m[0] + tp[at + 1, rows[i]] * m[1]
                        + tp[at + 2, rows[i]] * m[2]
                    )
            for i in range(parts):
                accs[3 * lb + g, rows[i]] = acc[i]
            return carry

        lax.fori_loop(0, lg * (BLOCK // CHUNK), grids, 0)

        for j in range(3 * lb + lg):
            nf[j] = jnp.sum(jnp.transpose(accs[j]), axis=0, keepdims=True)

    def apply_far(k):
        table = tables[k]
        drain(table.at[pl.ds(0, ncell - 1)], recv_sem.at[S_TB + k])
        for c8 in range(ncell // 8):
            rows = table[pl.ds(c8 * 8, 8)].reshape(8, BLOCK)
            for n in range(7):
                fb[n, pl.ds(c8 * 8, 8)] = jnp.broadcast_to(rows[:, n : n + 1], (8, BLOCK))
        field = [[None] * lb for _ in range(3)]
        for b in range(lb):
            acc = [jnp.zeros((8, BLOCK), F32) for _ in range(3)]
            for c8 in range(ncell // 8):
                row = pl.ds(c8 * 8, 8)
                xx, xy, xz, yy, yz, zz, cx, cy, cz = [fd[b * 9 + n, row] for n in range(9)]
                q, mx, my, mz = [fb[n, row] for n in range(3, 7)]
                acc[0] = acc[0] + ((xx * mx + xy * my) + (xz * mz + cx * q))
                acc[1] = acc[1] + ((xy * mx + yy * my) + (yz * mz + cy * q))
                acc[2] = acc[2] + ((xz * mx + yz * my) + (zz * mz + cz * q))
            for a in range(3):
                field[a][b] = jnp.sum(acc[a], axis=0, keepdims=True) + nf[b * 3 + a]
        potential = []
        for g in range(lg):
            acc = jnp.zeros((8, BLOCK), F32)
            for c8 in range(ncell // 8):
                row = pl.ds(c8 * 8, 8)
                acc = acc + (
                    fp[g * 3, row] * fb[0, row] + fp[g * 3 + 1, row] * fb[1, row]
                    + fp[g * 3 + 2, row] * fb[2, row]
                )
            potential.append(jnp.sum(acc, axis=0, keepdims=True) + nf[3 * lb + g])
        mu = [
            [pol[0:1, lanes(b)] * (fixed[a : a + 1, lanes(b)] + field[a][b]) for b in range(lb)]
            for a in range(3)
        ]
        q = [base[0:1, lanes(g)] - resp[0:1, lanes(g)] * potential[g] for g in range(lg)]
        return mu, q

    share_sums(0)
    share_group(pos, own * prows, prows, S_POS)
    share_state(0)
    for k in range(ITERS):
        share_cell(k)
        if k == 0:
            forward(pos, prows, S_POS, S_PL, S_PR)
        forward(windows[k], urows, S_W + k, S_FL + k, S_FR + k)
        if k == 0:
            arrived(pos, prows, S_PL, S_PR)
            build()
        arrived(windows[k], urows, S_FL + k, S_FR + k)
        apply_near(windows[k])
        mu, q = apply_far(k)
        if k < ITERS - 1:
            put_state(k + 1, mu, q)
            share_sums(k + 1)
            share_state(k + 1)
        else:
            for a in range(3):
                for b in range(lb):
                    out_mu[a : a + 1, lanes(b)] = mu[a][b]
            for g in range(lg):
                out_q[0:1, lanes(g)] = q[g]

    def sent(ref, rows, sem_group, sem_left, sem_right):
        size = ngrp * rows
        drain(ref.at[pl.ds(0, (ngrp - 1) * rows)], send_sem.at[sem_group])

        @pl.when(cell < ncell - 1)
        def _():
            drain(ref.at[pl.ds(0, size)], send_sem.at[sem_right])

        @pl.when(cell > 0)
        def _():
            drain(ref.at[pl.ds(0, size)], send_sem.at[sem_left])

    sent(pos, prows, S_POS, S_PL, S_PR)
    for k in range(ITERS):
        drain(sa.at[pl.ds(0, ngrp - 1)], send_sem.at[S_SA + k])
        drain(tables[k].at[pl.ds(0, ncell - 1)], send_sem.at[S_TB + k])
        sent(windows[k], urows, S_W + k, S_FL + k, S_FR + k)


def body(
    ncell, ngrp,
    atom_sites, grid_points, dipole_guess, fixed_field, polarisability, base_charge, response,
    near_blocks, grid_blocks, source_blocks,
):
    lb, nb = near_blocks.shape
    nq = grid_blocks.shape[1]
    lg, nm = source_blocks.shape
    urows = 3 * lb + lg
    prows = 3 * lb + 3 * lg
    vmem = pl.BlockSpec(memory_space=pltpu.VMEM)
    smem = pl.BlockSpec(memory_space=pltpu.SMEM)
    tile = (BLOCK, BLOCK)
    window = pltpu.VMEM((3 * ngrp * urows, 1, BLOCK), F32)
    table = pltpu.VMEM((ncell, 1, BLOCK), F32)
    mu, q = pl.pallas_call(
        functools.partial(kernel, ncell, ngrp, lb, lg, nb, nq, nm),
        out_shape=(
            jax.ShapeDtypeStruct((3, lb * BLOCK), F32),
            jax.ShapeDtypeStruct((1, lg * BLOCK), F32),
        ),
        in_specs=[smem] * 3 + [vmem] * 7,
        out_specs=(vmem, vmem),
        scratch_shapes=[
            window, window, window,
            pltpu.VMEM((3 * ngrp * prows, 1, BLOCK), F32),
            pltpu.VMEM((ITERS * ngrp, 1, BLOCK), F32),
            table, table, table,
            pltpu.VMEM(((lb + lg) * 3, *tile), F32),
            pltpu.VMEM((lb * (nb + 1) * 6, *tile), F32),
            pltpu.VMEM((lb * nq * 3, *tile), F32),
            pltpu.VMEM((lg * nm * 3, *tile), F32),
            pltpu.VMEM((lb * 9, ncell, BLOCK), F32),
            pltpu.VMEM((lg * 3, ncell, BLOCK), F32),
            pltpu.VMEM((7, ncell, BLOCK), F32),
            pltpu.VMEM((lb * (nb + 1) * 3, 8, BLOCK), F32),
            pltpu.VMEM((lg * nm * 3, 8, BLOCK), F32),
            pltpu.VMEM((lb * nq, 8, BLOCK), F32),
            pltpu.VMEM((3 * lb + lg, *tile), F32),
            pltpu.VMEM((3 * lb + lg, 1, BLOCK), F32),
            pltpu.VMEM((8, BLOCK), F32),
            pltpu.SemaphoreType.DMA((18,)),
            pltpu.SemaphoreType.DMA((18,)),
        ],
        compiler_params=pltpu.CompilerParams(
            collective_id=0, has_side_effects=True, vmem_limit_bytes=60 * 1024 * 1024
        ),
    )(
        near_blocks, grid_blocks, source_blocks,
        atom_sites, grid_points, dipole_guess, fixed_field,
        polarisability.reshape(1, -1), base_charge.reshape(1, -1), response.reshape(1, -1),
    )
    return mu, q.reshape(-1)


def solution(mesh):
    shared = P(None, ("cell", "grp"))
    flat = P(("cell", "grp"))
    rows = P(("cell", "grp"), None)
    return jax.shard_map(
        functools.partial(body, mesh.shape["cell"], mesh.shape["grp"]),
        mesh=mesh,
        in_specs=(shared, shared, shared, shared, flat, flat, flat, rows, rows, rows),
        out_specs=(shared, flat),
        check_vma=False,
    )
```

```python
import functools

import jax
import jax.numpy as jnp
from jax import lax
from jax.experimental import pallas as pl
from jax.experimental.pallas import tpu as pltpu
from jax.sharding import PartitionSpec as P

BLOCK = 128
ITERS = 3
CHUNK = 32
SOFT = 0.04
ROOT3 = 3.0**0.5
MESH = pl.DeviceIdType.MESH
F32 = jnp.float32


def copy_to(src, dst, send_sem, recv_sem, device):
    pltpu.make_async_remote_copy(
        src_ref=src,
        dst_ref=dst,
        send_sem=send_sem,
        recv_sem=recv_sem,
        device_id=device,
        device_id_type=MESH,
    ).start()


def drain(ref, sem):
    pltpu.make_async_copy(ref, ref, sem).wait()


def ring_order(size):
    return sorted(range(1, size), key=lambda d: -min(d, size - d))


def far_order(ncell):
    def hops(d):
        total = 0
        for c in range(ncell):
            a, b = c // 2, (c + d) % ncell // 2
            dz, dx = abs(a % 8 - b % 8), abs(a // 8 - b // 8)
            total += min(dz, 8 - dz) + min(dx, ncell // 16 - dx)
        return total

    return sorted(range(1, ncell), key=lambda d: (-hops(d), d))


def powers(dx, dy, dz):
    s = lax.rsqrt(dx * dx + dy * dy + dz * dz + SOFT)
    return s, s * s * s


def pair_tensor(dx, dy, dz, s3, s5):
    t = 3.0 * s5
    tx, ty, tz = t * dx, t * dy, t * dz
    return (tx * dx - s3, tx * dy, tx * dz, ty * dy - s3, ty * dz, tz * dz - s3)


def kernel(
    ncell, ngrp, lb, lg, nb, nq, nm,
    near_in, grid_in, source_in,
    sites_in, points_in, guess_in, fixed_in, pol_in, base_in, resp_in,
    out_mu, out_q,
    near_list, grid_list, source_list,
    sites, points, guess, fixed, pol, base, resp,
    urow, prow,
    w0, w1, w2, pos, sa, tb0, tb1, tb2,
    tgt, td, tc, tp, fd, fp, fb, mub, accs, nf,
    local_sem, send_sem, recv_sem,
):
    windows = (w0, w1, w2)
    tables = (tb0, tb1, tb2)
    cell = lax.axis_index("cell")
    grp = lax.axis_index("grp")
    urows = 3 * lb + lg
    prows = 3 * lb + 3 * lg
    slots = nb + 1
    own = ngrp + grp

    loads = [
        pltpu.make_async_copy(src, dst, local_sem.at[n])
        for n, (src, dst) in enumerate(
            (
                (sites_in, sites), (points_in, points), (guess_in, guess), (base_in, base),
                (near_in, near_list), (grid_in, grid_list), (source_in, source_list),
                (fixed_in, fixed), (pol_in, pol), (resp_in, resp),
            )
        )
    ]
    for load in loads:
        load.start()
    others = far_order(ncell)

    def cell_at(d):
        return (cell + d) & (ncell - 1)

    def group_at(d):
        return (grp + d) & (ngrp - 1)

    barrier = pltpu.get_barrier_semaphore()
    with jax.named_scope("greet"):
        for d in others:
            pl.semaphore_signal(
                barrier, inc=1, device_id=(cell_at(d), grp), device_id_type=MESH
            )
        for d in ring_order(ngrp):
            pl.semaphore_signal(
                barrier, inc=1, device_id=(cell, group_at(d)), device_id_type=MESH
            )
    for load in loads:
        load.wait()

    def lanes(j):
        return pl.ds(j * BLOCK, BLOCK)

    zc = [cell.astype(F32) + 0.5, 0.5, 0.5]
    lane = lax.broadcasted_iota(jnp.int32, (1, BLOCK), 1)

    def put_state(k, mu, q):
        w = windows[k]
        for a in range(3):
            for b in range(lb):
                w[own * urows + a * lb + b] = mu[a][b]
        for g in range(lg):
            w[own * urows + 3 * lb + g] = q[g]
        sums = [functools.reduce(jnp.add, mu[a]) for a in range(3)]
        sums.append(functools.reduce(jnp.add, q))
        for a in range(3):
            moment = functools.reduce(
                jnp.add, [q[g] * (points[a : a + 1, lanes(g)] - zc[a]) for g in range(lg)]
            )
            sums.append(moment + sums[a])
        row = jnp.zeros((1, BLOCK), F32)
        for n, s in enumerate(sums):
            row = jnp.where(lane == n, jnp.sum(s, axis=1, keepdims=True), row)
        sa[k * ngrp + grp] = row

    for a in range(3):
        for b in range(lb):
            pos[own * prows + a * lb + b] = sites[a : a + 1, lanes(b)]
        for g in range(lg):
            pos[own * prows + 3 * lb + a * lg + g] = points[a : a + 1, lanes(g)]
    put_state(
        0,
        [[guess[a : a + 1, lanes(b)] for b in range(lb)] for a in range(3)],
        [base[g : g + 1] for g in range(lg)],
    )

    def atom_rows(n, w):
        at, b = lax.shift_right_logical(w, lb.bit_length() - 1), w & (lb - 1)
        urow[n] = at * urows + b
        prow[n] = at * prows + b

    def grid_rows(n, w):
        at = w // lg
        b = w - at * lg
        urow[n] = at * urows + 3 * lb + b
        prow[n] = at * prows + 3 * lb + b

    A_GRID = lb * slots
    A_SRC = A_GRID + lb * nq
    for b in range(lb):
        atom_rows(b * slots, own * lb + b)
        for s in range(nb):
            atom_rows(b * slots + 1 + s, near_list[b, s])
        for s in range(nq):
            grid_rows(A_GRID + b * nq + s, grid_list[b, s])
    for g in range(lg):
        for s in range(nm):
            atom_rows(A_SRC + g * nm + s, source_list[g, s])

    def clear(start):
        for w in windows:
            w[pl.ds(start * ngrp * urows, ngrp * urows)] = jnp.zeros(
                (ngrp * urows, 1, BLOCK), F32
            )
        pos[pl.ds(start * ngrp * prows, ngrp * prows)] = jnp.zeros((ngrp * prows, 1, BLOCK), F32)

    @pl.when(cell == 0)
    def _():
        clear(0)

    @pl.when(cell == ncell - 1)
    def _():
        clear(2)

    for a in range(3):
        for b in range(lb):
            tgt[b * 3 + a] = jnp.transpose(
                jnp.broadcast_to(sites[a : a + 1, lanes(b)], (BLOCK, BLOCK))
            )
        for g in range(lg):
            tgt[(lb + g) * 3 + a] = jnp.transpose(
                jnp.broadcast_to(points[a : a + 1, lanes(g)], (BLOCK, BLOCK))
            )

    cells8 = lax.broadcasted_iota(jnp.int32, (8, BLOCK), 0)

    def far_rows(ref, j, c8):
        number = cells8 + c8 * 8
        dx = ref[0:1, lanes(j)] - (number.astype(F32) + 0.5)
        dy = ref[1:2, lanes(j)] - 0.5 + jnp.zeros_like(dx)
        dz = ref[2:3, lanes(j)] - 0.5 + jnp.zeros_like(dx)
        keep = jnp.abs(number - cell) >= 2
        s1, s3 = powers(dx, dy, dz)
        s3 = jnp.where(keep, s3, 0.0)
        return dx, dy, dz, s3, s3 * s1 * s1

    def far_build(c8, carry):
        row = pl.ds(pl.multiple_of(c8 * 8, 8), 8)
        for b in range(lb):
            dx, dy, dz, s3, s5 = far_rows(sites, b, c8)
            for n, v in enumerate(pair_tensor(dx, dy, dz, s3, s5)):
                fd[b * 9 + n, row] = v
            for n, v in enumerate((dx, dy, dz)):
                fd[b * 9 + 6 + n, row] = v * s3
        for g in range(lg):
            dx, dy, dz, s3, s5 = far_rows(points, g, c8)
            for n, v in enumerate((dx, dy, dz)):
                fp[g * 3 + n, row] = v * s3
        return carry

    with jax.named_scope("far_build"):
        lax.fori_loop(0, ncell // 8, far_build, 0)

    with jax.named_scope("barrier"):
        pl.semaphore_wait(barrier, ncell + ngrp - 2)

    S_SA, S_W, S_FL, S_FR, S_TB = 0, 3, 6, 9, 12
    S_POS, S_PL, S_PR = 15, 16, 17

    def share_group(ref, start, count, sem):
        part = ref.at[pl.ds(start, count)]
        for d in ring_order(ngrp):
            copy_to(part, part, send_sem.at[sem], recv_sem.at[sem], (cell, group_at(d)))

    def share_sums(k):
        share_group(sa, k * ngrp + grp, 1, S_SA + k)

    def share_state(k):
        share_group(windows[k], own * urows, urows, S_W + k)

    def share_cell(k):
        drain(sa.at[pl.ds(0, ngrp - 1)], recv_sem.at[S_SA + k])
        total = functools.reduce(jnp.add, [sa[k * ngrp + j] for j in range(ngrp)])
        table = tables[k]
        table[cell] = total

        part = table.at[pl.ds(cell, 1)]
        for d in others:
            copy_to(
                part, part, send_sem.at[S_TB + k], recv_sem.at[S_TB + k], (cell_at(d), grp)
            )

    def forward(ref, rows, sem_group, sem_left, sem_right):
        drain(ref.at[pl.ds(0, (ngrp - 1) * rows)], recv_sem.at[sem_group])
        size = ngrp * rows
        mine = ref.at[pl.ds(size, size)]

        @pl.when(cell < ncell - 1)
        def _():
            copy_to(
                mine, ref.at[pl.ds(0, size)],
                send_sem.at[sem_right], recv_sem.at[sem_right], (cell + 1, grp),
            )

        @pl.when(cell > 0)
        def _():
            copy_to(
                mine, ref.at[pl.ds(2 * size, size)],
                send_sem.at[sem_left], recv_sem.at[sem_left], (cell - 1, grp),
            )

    def arrived(ref, rows, sem_left, sem_right):
        size = ngrp * rows

        @pl.when(cell > 0)
        def _():
            drain(ref.at[pl.ds(0, size)], recv_sem.at[sem_right])

        @pl.when(cell < ncell - 1)
        def _():
            drain(ref.at[pl.ds(2 * size, size)], recv_sem.at[sem_left])

    tiles = BLOCK // 8

    def tile(t):
        return pl.ds(8 * t, 8)

    def wide(row):
        return jnp.broadcast_to(row, (8, BLOCK))

    def build():
        diagonal = lax.broadcasted_iota(jnp.int32, (8, BLOCK), 1) - lax.broadcasted_iota(
            jnp.int32, (8, BLOCK), 0
        )

        def deltas(j, t, rows):
            return [tgt[j * 3 + a, tile(t)] - rows[a] for a in range(3)]

        def dipole_slot(b, n, own_block):
            r = prow[n]
            rows = [wide(pos[r + a * lb]) for a in range(3)]
            for t in range(tiles):
                dx, dy, dz = deltas(b, t, rows)
                s1, s3 = powers(dx, dy, dz)
                w = ROOT3 * (s3 * lax.rsqrt(s1))
                if own_block:
                    s3 = jnp.where(diagonal == 8 * t, 0.0, s3)
                for i, v in enumerate((w * dx, w * dy, w * dz, s3)):
                    td[n * 4 + i, tile(t)] = v

        def charge_slot(ref, j, n, at, step):
            r = prow[n]
            rows = [wide(pos[r + a * step]) for a in range(3)]
            for t in range(tiles):
                dx, dy, dz = deltas(j, t, rows)
                _, s3 = powers(dx, dy, dz)
                for i, v in enumerate((dx, dy, dz)):
                    ref[at * 3 + i, tile(t)] = v * s3

        def atoms(b, carry):
            dipole_slot(b, b * slots, True)

            def pair(i, c):
                dipole_slot(b, b * slots + 1 + 2 * i, False)
                dipole_slot(b, b * slots + 2 + 2 * i, False)
                return c

            lax.fori_loop(0, nb // 2, pair, 0)

            def charge(i, c):
                for e in range(2):
                    at = b * nq + 2 * i + e
                    charge_slot(tc, b, A_GRID + at, at, lg)
                return c

            lax.fori_loop(0, nq // 2, charge, 0)
            return carry

        lax.fori_loop(0, lb, atoms, 0)

        def grids(i, carry):
            g = i // (nm // 2)
            for e in range(2):
                at = 2 * i + e
                charge_slot(tp, lb + g, A_SRC + at, at, lb)
            return carry

        lax.fori_loop(0, lg * nm // 2, grids, 0)

    def reduce_rows(j):
        nf[j] = jnp.sum(jnp.transpose(accs[j]), axis=0, keepdims=True)

    def apply_near(w):
        parts = CHUNK // 8

        def atoms(b, carry):
            for s in range(slots):
                r = urow[b * slots + s]
                for a in range(3):
                    mub[s * 3 + a] = wide(w[r + a * lb])
            for s in range(nq):
                mub[slots * 3 + s] = wide(w[urow[A_GRID + b * nq + s]])
            before = jnp.maximum(b - 1, 0)
            for c in range(BLOCK // CHUNK):
                rows = [tile(c * parts + i) for i in range(parts)]
                acc = [[jnp.zeros((8, BLOCK), F32) for _ in range(parts)] for _ in range(3)]
                for s in range(slots):
                    m = [mub[s * 3 + a] for a in range(3)]
                    at = (b * slots + s) * 4
                    for i in range(parts):
                        vx, vy, vz, s3 = [td[at + n, rows[i]] for n in range(4)]
                        p = vx * m[0] + vy * m[1] + vz * m[2]
                        for a, v in enumerate((vx, vy, vz)):
                            acc[a][i] = acc[a][i] + (v * p - s3 * m[a])
                for s in range(nq):
                    q = mub[slots * 3 + s]
                    for i in range(parts):
                        for a in range(3):
                            acc[a][i] = acc[a][i] + tc[(b * nq + s) * 3 + a, rows[i]] * q
                for a in range(3):
                    for i in range(parts):
                        accs[b * 3 + a, rows[i]] = acc[a][i]
                if c < 3:
                    reduce_rows(before * 3 + c)
            return carry

        lax.fori_loop(0, lb, atoms, 0)

        def grids(g, carry):
            for s in range(nm):
                r = urow[A_SRC + g * nm + s]
                for a in range(3):
                    mub[s * 3 + a] = wide(w[r + a * lb])
            for c in range(BLOCK // CHUNK):
                rows = [tile(c * parts + i) for i in range(parts)]
                acc = [jnp.zeros((8, BLOCK), F32) for _ in range(parts)]
                for s in range(nm):
                    m = [mub[s * 3 + a] for a in range(3)]
                    at = (g * nm + s) * 3
                    for i in range(parts):
                        acc[i] = acc[i] + (
                            tp[at, rows[i]] * m[0] + tp[at + 1, rows[i]] * m[1]
                            + tp[at + 2, rows[i]] * m[2]
                        )
                for i in range(parts):
                    accs[3 * lb + g, rows[i]] = acc[i]
            reduce_rows(3 * lb - 3 + g)
            return carry

        lax.fori_loop(0, lg, grids, 0)
        for g in range(lg):
            reduce_rows(3 * lb + g)

    def apply_far(k):
        table = tables[k]
        for c8 in range(ncell // 8):
            rows = table[pl.ds(c8 * 8, 8)].reshape(8, BLOCK)
            for n in range(7):
                fb[n, pl.ds(c8 * 8, 8)] = jnp.broadcast_to(rows[:, n : n + 1], (8, BLOCK))
        field = [[None] * lb for _ in range(3)]
        for b in range(lb):
            acc = [jnp.zeros((8, BLOCK), F32) for _ in range(3)]
            for c8 in range(ncell // 8):
                row = pl.ds(c8 * 8, 8)
                xx, xy, xz, yy, yz, zz, cx, cy, cz = [fd[b * 9 + n, row] for n in range(9)]
                q, mx, my, mz = [fb[n, row] for n in range(3, 7)]
                acc[0] = acc[0] + ((xx * mx + xy * my) + (xz * mz + cx * q))
                acc[1] = acc[1] + ((xy * mx + yy * my) + (yz * mz + cy * q))
                acc[2] = acc[2] + ((xz * mx + yz * my) + (zz * mz + cz * q))
            for a in range(3):
                field[a][b] = jnp.sum(acc[a], axis=0, keepdims=True) + nf[b * 3 + a]
        potential = []
        for g in range(lg):
            acc = jnp.zeros((8, BLOCK), F32)
            for c8 in range(ncell // 8):
                row = pl.ds(c8 * 8, 8)
                acc = acc + (
                    fp[g * 3, row] * fb[0, row] + fp[g * 3 + 1, row] * fb[1, row]
                    + fp[g * 3 + 2, row] * fb[2, row]
                )
            potential.append(jnp.sum(acc, axis=0, keepdims=True) + nf[3 * lb + g])
        return field, potential

    def new_state(field, potential):
        mu = [
            [pol[b : b + 1] * (fixed[a : a + 1, lanes(b)] + field[a][b]) for b in range(lb)]
            for a in range(3)
        ]
        q = [base[g : g + 1] - resp[g : g + 1] * potential[g] for g in range(lg)]
        return mu, q

    scope = jax.named_scope
    with scope("send0"):
        share_sums(0)
        share_group(pos, own * prows, prows, S_POS)
        share_state(0)
    for k in range(ITERS):
        with scope(f"share_cell#k={k}"):
            share_cell(k)
        with scope(f"forward#k={k}"):
            if k == 0:
                forward(pos, prows, S_POS, S_PL, S_PR)
            forward(windows[k], urows, S_W + k, S_FL + k, S_FR + k)
        if k == 0:
            with scope("wait_pos"):
                arrived(pos, prows, S_PL, S_PR)
            with scope("build"):
                build()
        with scope(f"wait_window#k={k}"):
            arrived(windows[k], urows, S_FL + k, S_FR + k)
        with scope(f"near#k={k}"):
            apply_near(windows[k])
        with scope(f"wait_far#k={k}"):
            drain(tables[k].at[pl.ds(0, ncell - 1)], recv_sem.at[S_TB + k])
        with scope(f"far#k={k}"):
            field, potential = apply_far(k)
        if k < ITERS - 1:
            with scope(f"put#k={k}"):
                put_state(k + 1, *new_state(field, potential))
            with scope(f"send#k={k + 1}"):
                share_sums(k + 1)
                share_state(k + 1)
        else:
            mu, q = new_state(field, potential)
            for a in range(3):
                for b in range(lb):
                    out_mu[a : a + 1, lanes(b)] = mu[a][b]
            for g in range(lg):
                out_q[g : g + 1] = q[g]

    def sent(ref, rows, sem_group, sem_left, sem_right):
        size = ngrp * rows
        drain(ref.at[pl.ds(0, (ngrp - 1) * rows)], send_sem.at[sem_group])

        @pl.when(cell < ncell - 1)
        def _():
            drain(ref.at[pl.ds(0, size)], send_sem.at[sem_right])

        @pl.when(cell > 0)
        def _():
            drain(ref.at[pl.ds(0, size)], send_sem.at[sem_left])

    sent(pos, prows, S_POS, S_PL, S_PR)
    for k in range(ITERS):
        drain(sa.at[pl.ds(0, ngrp - 1)], send_sem.at[S_SA + k])
        drain(tables[k].at[pl.ds(0, ncell - 1)], send_sem.at[S_TB + k])
        sent(windows[k], urows, S_W + k, S_FL + k, S_FR + k)


def body(
    ncell, ngrp,
    atom_sites, grid_points, dipole_guess, fixed_field, polarisability, base_charge, response,
    near_blocks, grid_blocks, source_blocks,
):
    lb, nb = near_blocks.shape
    nq = grid_blocks.shape[1]
    lg, nm = source_blocks.shape
    urows = 3 * lb + lg
    prows = 3 * lb + 3 * lg
    vmem = pl.BlockSpec(memory_space=pltpu.VMEM)
    tile = (BLOCK, BLOCK)
    window = pltpu.VMEM((3 * ngrp * urows, 1, BLOCK), F32)
    table = pltpu.VMEM((ncell, 1, BLOCK), F32)
    mu, q = pl.pallas_call(
        functools.partial(kernel, ncell, ngrp, lb, lg, nb, nq, nm),
        out_shape=(
            pltpu.VMEM((3, lb * BLOCK), F32),
            pltpu.VMEM((lg, BLOCK), F32),
        ),
        in_specs=[pl.BlockSpec(memory_space=pl.ANY)] * 10,
        out_specs=(vmem, vmem),
        scratch_shapes=[
            pltpu.SMEM(near_blocks.shape, jnp.int32),
            pltpu.SMEM(grid_blocks.shape, jnp.int32),
            pltpu.SMEM(source_blocks.shape, jnp.int32),
            pltpu.VMEM((3, lb * BLOCK), F32),
            pltpu.VMEM((3, lg * BLOCK), F32),
            pltpu.VMEM((3, lb * BLOCK), F32),
            pltpu.VMEM((3, lb * BLOCK), F32),
            pltpu.VMEM((lb, BLOCK), F32),
            pltpu.VMEM((lg, BLOCK), F32),
            pltpu.VMEM((lg, BLOCK), F32),
            pltpu.SMEM((lb * (nb + 1 + nq) + lg * nm,), jnp.int32),
            pltpu.SMEM((lb * (nb + 1 + nq) + lg * nm,), jnp.int32),
            window, window, window,
            pltpu.VMEM((3 * ngrp * prows, 1, BLOCK), F32),
            pltpu.VMEM((ITERS * ngrp, 1, BLOCK), F32),
            table, table, table,
            pltpu.VMEM(((lb + lg) * 3, *tile), F32),
            pltpu.VMEM((lb * (nb + 1) * 4, *tile), F32),
            pltpu.VMEM((lb * nq * 3, *tile), F32),
            pltpu.VMEM((lg * nm * 3, *tile), F32),
            pltpu.VMEM((lb * 9, ncell, BLOCK), F32),
            pltpu.VMEM((lg * 3, ncell, BLOCK), F32),
            pltpu.VMEM((7, ncell, BLOCK), F32),
            pltpu.VMEM(((nb + 1) * 3 + nq, 8, BLOCK), F32),
            pltpu.VMEM((3 * lb + lg, *tile), F32),
            pltpu.VMEM((3 * lb + lg, 1, BLOCK), F32),
            pltpu.SemaphoreType.DMA((10,)),
            pltpu.SemaphoreType.DMA((18,)),
            pltpu.SemaphoreType.DMA((18,)),
        ],
        compiler_params=pltpu.CompilerParams(
            collective_id=0, has_side_effects=True, vmem_limit_bytes=60 * 1024 * 1024
        ),
    )(
        near_blocks, grid_blocks, source_blocks,
        atom_sites, grid_points, dipole_guess, fixed_field,
        polarisability.reshape(lb, BLOCK), base_charge.reshape(lg, BLOCK),
        response.reshape(lg, BLOCK),
    )
    return mu, q.reshape(-1)


def solution(mesh):
    shared = P(None, ("cell", "grp"))
    flat = P(("cell", "grp"))
    rows = P(("cell", "grp"), None)
    return jax.shard_map(
        functools.partial(body, mesh.shape["cell"], mesh.shape["grp"]),
        mesh=mesh,
        in_specs=(shared, shared, shared, shared, flat, flat, flat, rows, rows, rows),
        out_specs=(shared, flat),
        check_vma=False,
    )
```

```python
import functools

import jax
import jax.numpy as jnp
from jax import lax
from jax.experimental import pallas as pl
from jax.experimental.pallas import tpu as pltpu
from jax.sharding import PartitionSpec as P

BLOCK = 128
ITERS = 3
CHUNK = 32
SOFT = 0.04
ROOT3 = 3.0**0.5
DIRECT_P = False
DIRECT_W = (False, True, True)
MESH = pl.DeviceIdType.MESH
F32 = jnp.float32


def copy_to(src, dst, send_sem, recv_sem, device):
    pltpu.make_async_remote_copy(
        src_ref=src,
        dst_ref=dst,
        send_sem=send_sem,
        recv_sem=recv_sem,
        device_id=device,
        device_id_type=MESH,
    ).start()


def drain(ref, sem):
    pltpu.make_async_copy(ref, ref, sem).wait()


def ring_order(size):
    return sorted(range(1, size), key=lambda d: -min(d, size - d))


def far_order(ncell):
    def hops(d):
        total = 0
        for c in range(ncell):
            a, b = c // 2, (c + d) % ncell // 2
            dz, dx = abs(a % 8 - b % 8), abs(a // 8 - b // 8)
            total += min(dz, 8 - dz) + min(dx, ncell // 16 - dx)
        return total

    return sorted(range(1, ncell), key=lambda d: (-hops(d), d))


def powers(dx, dy, dz):
    s = lax.rsqrt(dx * dx + dy * dy + dz * dz + SOFT)
    return s, s * s * s


def pair_tensor(dx, dy, dz, s3, s5):
    t = 3.0 * s5
    tx, ty, tz = t * dx, t * dy, t * dz
    return (tx * dx - s3, tx * dy, tx * dz, ty * dy - s3, ty * dz, tz * dz - s3)


def kernel(
    ncell, ngrp, lb, lg, nb, nq, nm,
    near_in, grid_in, source_in,
    sites_in, points_in, guess_in, fixed_in, pol_in, base_in, resp_in,
    out_mu, out_q,
    near_list, grid_list, source_list,
    sites, points, guess, fixed, pol, base, resp,
    urow, prow,
    w0, w1, w2, pos, sa, tb0, tb1, tb2,
    tgt, td, tc, tp, fd, fp, zst, lin, lint, tab, mub, accs, nf,
    local_sem, send_sem, recv_sem, hello,
):
    windows = (w0, w1, w2)
    tables = (tb0, tb1, tb2)
    cell = lax.axis_index("cell")
    grp = lax.axis_index("grp")
    urows = 3 * lb + lg
    prows = 3 * lb + 3 * lg
    slots = nb + 1
    own = ngrp + grp

    others = far_order(ncell)

    def cell_at(d):
        return (cell + d) & (ncell - 1)

    def group_at(d):
        return (grp + d) & (ngrp - 1)

    def signal(sem, to_cell, to_grp):
        pl.semaphore_signal(sem, inc=1, device_id=(to_cell, to_grp), device_id_type=MESH)

    beside = cell_at(2 * (cell & 1) - 1)
    partner = cell ^ 1
    line = cell & 14
    z_line = [(cell - line) + ((line + 2 * d) & 14) for d in ring_order(8)]
    x_line = [cell_at(16 * d) for d in range(1, ncell // 16)]
    barrier = pltpu.get_barrier_semaphore()
    with jax.named_scope("greet"):
        for d in ring_order(ngrp):
            signal(barrier, cell, group_at(d))
        for other in z_line + x_line + [beside, partner]:
            signal(barrier, other, grp)
    greeted = ngrp - 1 + len(z_line) + len(x_line) + 2
    loads = [
        pltpu.make_async_copy(src, dst, local_sem.at[n])
        for n, (src, dst) in enumerate(
            (
                (sites_in, sites), (points_in, points), (guess_in, guess), (base_in, base),
                (near_in, near_list), (grid_in, grid_list), (source_in, source_list),
                (fixed_in, fixed), (pol_in, pol), (resp_in, resp),
            )
        )
    ]
    for load in loads:
        load.start()
    for load in loads:
        load.wait()

    tiles = BLOCK // 8

    def tile(t):
        return pl.ds(8 * t, 8)

    def lanes(j):
        return pl.ds(j * BLOCK, BLOCK)

    zc = [cell.astype(F32) + 0.5, 0.5, 0.5]
    lane = lax.broadcasted_iota(jnp.int32, (1, BLOCK), 1)

    def put_sums(k, mu, q):
        sums = [functools.reduce(jnp.add, mu[a]) for a in range(3)]
        sums.append(functools.reduce(jnp.add, q))
        for a in range(3):
            moment = functools.reduce(jnp.add, [q[g] * offsets(a, g) for g in range(lg)])
            sums.append(moment + sums[a])
        row = jnp.zeros((1, BLOCK), F32)
        for n, total in enumerate(sums):
            row = jnp.where(lane == n, jnp.sum(total, axis=1, keepdims=True), row)
        sa[k * ngrp + grp] = row

    def put_state(k, mu, q):
        w = windows[k]
        for a in range(3):
            for b in range(lb):
                w[own * urows + a * lb + b] = mu[a][b]
        for g in range(lg):
            w[own * urows + 3 * lb + g] = q[g]

    def offsets(a, g):
        return points[a : a + 1, lanes(g)] - zc[a]

    for a in range(3):
        for b in range(lb):
            pos[own * prows + a * lb + b] = sites[a : a + 1, lanes(b)]
        for g in range(lg):
            pos[own * prows + 3 * lb + a * lg + g] = points[a : a + 1, lanes(g)]
    first = (
        [[guess[a : a + 1, lanes(b)] for b in range(lb)] for a in range(3)],
        [base[g : g + 1] for g in range(lg)],
    )
    put_sums(0, *first)
    put_state(0, *first)

    def atom_rows(n, w):
        at, b = lax.shift_right_logical(w, lb.bit_length() - 1), w & (lb - 1)
        urow[n] = at * urows + b
        prow[n] = at * prows + b

    def grid_rows(n, w):
        at = w // lg
        b = w - at * lg
        urow[n] = at * urows + 3 * lb + b
        prow[n] = at * prows + 3 * lb + b

    A_GRID = lb * slots
    A_SRC = A_GRID + lb * nq
    for b in range(lb):
        atom_rows(b * slots, own * lb + b)
        for s in range(nb):
            atom_rows(b * slots + 1 + s, near_list[b, s])
        for s in range(nq):
            grid_rows(A_GRID + b * nq + s, grid_list[b, s])
    for g in range(lg):
        for s in range(nm):
            atom_rows(A_SRC + g * nm + s, source_list[g, s])

    def clear(start):
        for w in windows:
            w[pl.ds(start * ngrp * urows, ngrp * urows)] = jnp.zeros(
                (ngrp * urows, 1, BLOCK), F32
            )
        pos[pl.ds(start * ngrp * prows, ngrp * prows)] = jnp.zeros((ngrp * prows, 1, BLOCK), F32)

    @pl.when(cell == 0)
    def _():
        clear(0)

    @pl.when(cell == ncell - 1)
    def _():
        clear(2)

    S_SA, S_W, S_FL, S_FR, S_TB = 0, 3, 6, 9, 12
    S_POS, S_PL, S_PR, S_LIN = 15, 16, 17, 18

    def share_group(ref, start, count, sem):
        part = ref.at[pl.ds(start, count)]
        for d in ring_order(ngrp):
            copy_to(part, part, send_sem.at[sem], recv_sem.at[sem], (cell, group_at(d)))

    def share_sums(k):
        share_group(sa, k * ngrp + grp, 1, S_SA + k)

    def share_direct(ref, rows, sem_group, sem_left, sem_right):
        part = ref.at[pl.ds(own * rows, rows)]
        left = ref.at[pl.ds(grp * rows, rows)]
        right = ref.at[pl.ds((2 * ngrp + grp) * rows, rows)]
        for d in ring_order(ngrp):
            copy_to(
                part, part, send_sem.at[sem_group], recv_sem.at[sem_group], (cell, group_at(d))
            )

        beyond = ring_order(ngrp) + [0]

        @pl.when(((cell & 1) == 1) & (cell < ncell - 1))
        def _():
            for d in beyond:
                copy_to(
                    part, left,
                    send_sem.at[sem_right], recv_sem.at[sem_right], (cell + 1, group_at(d)),
                )

        @pl.when(((cell & 1) == 0) & (cell > 0))
        def _():
            for d in beyond:
                copy_to(
                    part, right,
                    send_sem.at[sem_left], recv_sem.at[sem_left], (cell - 1, group_at(d)),
                )

    def forward_partner(ref, rows, sem_group, sem_left, sem_right):
        drain(ref.at[pl.ds(0, (ngrp - 1) * rows)], recv_sem.at[sem_group])
        size = ngrp * rows
        mine = ref.at[pl.ds(size, size)]

        @pl.when((cell & 1) == 0)
        def _():
            copy_to(
                mine, ref.at[pl.ds(0, size)],
                send_sem.at[sem_right], recv_sem.at[sem_right], (cell + 1, grp),
            )

        @pl.when((cell & 1) == 1)
        def _():
            copy_to(
                mine, ref.at[pl.ds(2 * size, size)],
                send_sem.at[sem_left], recv_sem.at[sem_left], (cell - 1, grp),
            )

    def share_state(k):
        if DIRECT_W[k]:
            share_direct(windows[k], urows, S_W + k, S_FL + k, S_FR + k)
        else:
            share_group(windows[k], own * urows, urows, S_W + k)

    def share_cell(k, answer):
        drain(sa.at[pl.ds(0, ngrp - 1)], recv_sem.at[S_SA + k])
        total = functools.reduce(jnp.add, [sa[k * ngrp + j] for j in range(ngrp)])
        if answer is not None:
            total = total + answer
        table = tables[k]
        table[cell] = total

        part = table.at[pl.ds(cell, 1)]
        for d in others:
            copy_to(
                part, part, send_sem.at[S_TB + k], recv_sem.at[S_TB + k], (cell_at(d), grp)
            )

    def forward(ref, rows, sem_group, sem_left, sem_right):
        drain(ref.at[pl.ds(0, (ngrp - 1) * rows)], recv_sem.at[sem_group])
        size = ngrp * rows
        mine = ref.at[pl.ds(size, size)]

        @pl.when(cell < ncell - 1)
        def _():
            copy_to(
                mine, ref.at[pl.ds(0, size)],
                send_sem.at[sem_right], recv_sem.at[sem_right], (cell + 1, grp),
            )

        @pl.when(cell > 0)
        def _():
            copy_to(
                mine, ref.at[pl.ds(2 * size, size)],
                send_sem.at[sem_left], recv_sem.at[sem_left], (cell - 1, grp),
            )

    def arrived(ref, rows, sem_left, sem_right):
        size = ngrp * rows

        @pl.when(cell > 0)
        def _():
            drain(ref.at[pl.ds(0, size)], recv_sem.at[sem_right])

        @pl.when(cell < ncell - 1)
        def _():
            drain(ref.at[pl.ds(2 * size, size)], recv_sem.at[sem_left])

    def wide(row):
        return jnp.broadcast_to(row, (8, BLOCK))

    def build():
        diagonal = lax.broadcasted_iota(jnp.int32, (8, BLOCK), 1) - lax.broadcasted_iota(
            jnp.int32, (8, BLOCK), 0
        )

        def deltas(j, t, rows):
            return [tgt[j * 3 + a, tile(t)] - rows[a] for a in range(3)]

        def dipole_slot(b, n, own_block):
            r = prow[n]
            rows = [wide(pos[r + a * lb]) for a in range(3)]
            for t in range(tiles):
                dx, dy, dz = deltas(b, t, rows)
                s1, s3 = powers(dx, dy, dz)
                w = ROOT3 * (s3 * lax.rsqrt(s1))
                if own_block:
                    s3 = jnp.where(diagonal == 8 * t, 0.0, s3)
                for i, v in enumerate((w * dx, w * dy, w * dz, s3)):
                    td[n * 4 + i, tile(t)] = v

        def charge_slot(ref, j, n, at, step):
            r = prow[n]
            rows = [wide(pos[r + a * step]) for a in range(3)]
            for t in range(tiles):
                dx, dy, dz = deltas(j, t, rows)
                _, s3 = powers(dx, dy, dz)
                for i, v in enumerate((dx, dy, dz)):
                    ref[at * 3 + i, tile(t)] = v * s3

        def atoms(b, carry):
            dipole_slot(b, b * slots, True)

            def pair(i, c):
                dipole_slot(b, b * slots + 1 + 2 * i, False)
                dipole_slot(b, b * slots + 2 + 2 * i, False)
                return c

            lax.fori_loop(0, nb // 2, pair, 0)

            def charge(i, c):
                for e in range(2):
                    at = b * nq + 2 * i + e
                    charge_slot(tc, b, A_GRID + at, at, lg)
                return c

            lax.fori_loop(0, nq // 2, charge, 0)
            return carry

        lax.fori_loop(0, lb, atoms, 0)

        def grids(i, carry):
            g = i // (nm // 2)
            for e in range(2):
                at = 2 * i + e
                charge_slot(tp, lb + g, A_SRC + at, at, lb)
            return carry

        lax.fori_loop(0, lg * nm // 2, grids, 0)

    def reduce_rows(j):
        nf[j] = jnp.sum(jnp.transpose(accs[j]), axis=0, keepdims=True)

    def apply_near(w):
        parts = CHUNK // 8

        def atoms(b, carry):
            for s in range(slots):
                r = urow[b * slots + s]
                for a in range(3):
                    mub[s * 3 + a] = wide(w[r + a * lb])
            for s in range(nq):
                mub[slots * 3 + s] = wide(w[urow[A_GRID + b * nq + s]])
            before = jnp.maximum(b - 1, 0)
            for c in range(BLOCK // CHUNK):
                rows = [tile(c * parts + i) for i in range(parts)]
                acc = [[jnp.zeros((8, BLOCK), F32) for _ in range(parts)] for _ in range(3)]
                for s in range(slots):
                    m = [mub[s * 3 + a] for a in range(3)]
                    at = (b * slots + s) * 4
                    for i in range(parts):
                        vx, vy, vz, s3 = [td[at + n, rows[i]] for n in range(4)]
                        p = vx * m[0] + vy * m[1] + vz * m[2]
                        for a, v in enumerate((vx, vy, vz)):
                            acc[a][i] = acc[a][i] + (v * p - s3 * m[a])
                for s in range(nq):
                    q = mub[slots * 3 + s]
                    for i in range(parts):
                        for a in range(3):
                            acc[a][i] = acc[a][i] + tc[(b * nq + s) * 3 + a, rows[i]] * q
                for a in range(3):
                    for i in range(parts):
                        accs[b * 3 + a, rows[i]] = acc[a][i]
                if c < 3:
                    reduce_rows(before * 3 + c)
            return carry

        lax.fori_loop(0, lb, atoms, 0)

        def grids(g, carry):
            for s in range(nm):
                r = urow[A_SRC + g * nm + s]
                for a in range(3):
                    mub[s * 3 + a] = wide(w[r + a * lb])
            acc = [jnp.zeros((8, BLOCK), F32) for _ in range(tiles)]
            for s in range(nm):
                m = [mub[s * 3 + a] for a in range(3)]
                at = (g * nm + s) * 3
                for i in range(tiles):
                    acc[i] = acc[i] + (
                        tp[at, tile(i)] * m[0] + tp[at + 1, tile(i)] * m[1]
                        + tp[at + 2, tile(i)] * m[2]
                    )
            for i in range(tiles):
                accs[3 * lb + g, tile(i)] = acc[i]
            reduce_rows(3 * lb - 3 + g)
            return carry

        lax.fori_loop(0, lg, grids, 0)
        for g in range(lg):
            reduce_rows(3 * lb + g)

    def apply_far(k):
        table = tables[k]
        acc = [[jnp.zeros((8, BLOCK), F32) for _ in range(lb)] for _ in range(3)]
        pot = [jnp.zeros((8, BLOCK), F32) for _ in range(lg)]
        for c in range(ncell):
            tab[c : c + 1] = table[c]
        for c8 in range(ncell // 8):
            row = tile(c8)
            rows = tab[row]
            px, py, pz, q, mx, my, mz = [
                jnp.broadcast_to(rows[:, n : n + 1], (8, BLOCK)) for n in range(7)
            ]
            for b in range(lb):
                xx, xy, xz, yy, yz, zz, cx, cy, cz = [fd[b * 9 + n, row] for n in range(9)]
                acc[0][b] = acc[0][b] + ((xx * mx + xy * my) + (xz * mz + cx * q))
                acc[1][b] = acc[1][b] + ((xy * mx + yy * my) + (yz * mz + cy * q))
                acc[2][b] = acc[2][b] + ((xz * mx + yz * my) + (zz * mz + cz * q))
            for g in range(lg):
                pot[g] = pot[g] + (
                    fp[g * 3, row] * px + fp[g * 3 + 1, row] * py + fp[g * 3 + 2, row] * pz
                )
        field = [
            [jnp.sum(acc[a][b], axis=0, keepdims=True) + nf[b * 3 + a] for b in range(lb)]
            for a in range(3)
        ]
        potential = [
            jnp.sum(pot[g], axis=0, keepdims=True) + nf[3 * lb + g] for g in range(lg)
        ]
        return field, potential

    def far_answer():
        rows = tab[...]
        flat = jnp.transpose(jnp.concatenate([rows, rows], axis=0))
        px, py, pz, q, mx, my, mz = [flat[n : n + 1] for n in range(7)]
        left = lane < ncell
        halves = (
            jnp.where(left, mx, my), jnp.where(left, mz, q),
            jnp.where(left, px, py), jnp.where(left, pz, 0.0),
        )
        total = functools.reduce(jnp.add, [lint[t] * halves[t] for t in range(4)])
        total = jnp.sum(total, axis=1, keepdims=True)
        lanes8 = lax.broadcasted_iota(jnp.int32, (8, BLOCK), 1)
        return jnp.sum(jnp.where(lanes8 == cells8, total, 0.0), axis=0, keepdims=True)

    def near_state():
        none = [[nf[b * 3 + a] for b in range(lb)] for a in range(3)]
        return new_state(none, [nf[3 * lb + g] for g in range(lg)])

    def new_state(field, potential):
        mu = [
            [pol[b : b + 1] * (fixed[a : a + 1, lanes(b)] + field[a][b]) for b in range(lb)]
            for a in range(3)
        ]
        q = [base[g : g + 1] - resp[g : g + 1] * potential[g] for g in range(lg)]
        return mu, q

    scope = jax.named_scope
    with scope("barrier"):
        pl.semaphore_wait(barrier, greeted)
    signal(hello.at[0], beside, grp)
    for other in z_line:
        signal(hello.at[1], other, grp)
    with scope("send0"):
        share_sums(0)
        if DIRECT_P:
            share_direct(pos, prows, S_POS, S_PL, S_PR)
        else:
            share_group(pos, own * prows, prows, S_POS)
        share_state(0)
    for a in range(3):
        for b in range(lb):
            tgt[b * 3 + a] = jnp.transpose(
                jnp.broadcast_to(sites[a : a + 1, lanes(b)], (BLOCK, BLOCK))
            )
        for g in range(lg):
            tgt[(lb + g) * 3 + a] = jnp.transpose(
                jnp.broadcast_to(points[a : a + 1, lanes(g)], (BLOCK, BLOCK))
            )

    cells8 = lax.broadcasted_iota(jnp.int32, (8, BLOCK), 0)

    def far_rows(ref, j, c8):
        number = cells8 + c8 * 8
        dx = ref[0:1, lanes(j)] - (number.astype(F32) + 0.5)
        dy = ref[1:2, lanes(j)] - 0.5 + jnp.zeros_like(dx)
        dz = ref[2:3, lanes(j)] - 0.5 + jnp.zeros_like(dx)
        keep = jnp.abs(number - cell) >= 2
        s1, s3 = powers(dx, dy, dz)
        s3 = jnp.where(keep, s3, 0.0)
        return dx, dy, dz, s3, s3 * s1 * s1

    def far_build(c8, carry):
        row = pl.ds(pl.multiple_of(c8 * 8, 8), 8)
        low = pl.ds(pl.multiple_of(ncell + c8 * 8, 8), 8)
        answer = [jnp.zeros((8, BLOCK), F32) for _ in range(9)]
        for b in range(lb):
            dx, dy, dz, s3, s5 = far_rows(sites, b, c8)
            values = (*pair_tensor(dx, dy, dz, s3, s5), dx * s3, dy * s3, dz * s3)
            for n, v in enumerate(values):
                fd[b * 9 + n, row] = v
                answer[n] = answer[n] + v * pol[b : b + 1]
        charge = [[jnp.zeros((8, BLOCK), F32) for _ in range(3)] for _ in range(4)]
        for g in range(lg):
            dx, dy, dz, s3, s5 = far_rows(points, g, c8)
            for n, v in enumerate((dx, dy, dz)):
                fp[g * 3 + n, row] = v * s3
                change = v * s3 * resp[g : g + 1]
                charge[0][n] = charge[0][n] - change
                for a in range(3):
                    charge[1 + a][n] = charge[1 + a][n] - change * offsets(a, g)
        xx, xy, xz, yy, yz, zz, cx, cy, cz = answer
        halves = [(xx, xy), (xy, yy), (xz, yz), (xz, cx), (yz, cy), (zz, cz)]
        halves += [(c[0], c[1]) for c in charge]
        halves += [(c[2], jnp.zeros((8, BLOCK), F32)) for c in charge]
        for n, (top, bottom) in enumerate(halves):
            zst[n, row] = top
            zst[n, low] = bottom
        return carry

    with jax.named_scope("far_build"):
        lax.fori_loop(0, ncell // 8, far_build, 0)
        places = [
            [(a, a) for a in range(3)] + [(4 + a, a) for a in range(3)],
            [(a, 3 + a) for a in range(3)] + [(4 + a, 3 + a) for a in range(3)],
            [(3 + a, 6 + a) for a in range(4)],
            [(3 + a, 10 + a) for a in range(4)],
        ]
        flat = [jnp.sum(jnp.transpose(zst[n]), axis=0, keepdims=True) for n in range(14)]
        for t in range(4):
            value = jnp.zeros((8, BLOCK), F32)
            for at, n in places[t]:
                value = jnp.where(cells8 == at, flat[n], value)
            lin[grp, t] = value

    with scope("hello"):
        pl.semaphore_wait(hello.at[1], len(z_line))
        signal(hello.at[2], partner, grp)
        pl.semaphore_wait(hello.at[2], 1)
        pl.semaphore_wait(hello.at[0], 1)
    answer = None
    for k in range(ITERS):
        with scope(f"share_cell#k={k}"):
            share_cell(k, answer)
        with scope(f"forward#k={k}"):
            if k == 0:
                (forward_partner if DIRECT_P else forward)(pos, prows, S_POS, S_PL, S_PR)
            (forward_partner if DIRECT_W[k] else forward)(
                windows[k], urows, S_W + k, S_FL + k, S_FR + k
            )
        if k == 0:
            for d in ring_order(ngrp):
                copy_to(
                    lin.at[grp], lin.at[grp], send_sem.at[S_LIN], recv_sem.at[S_LIN],
                    (cell, group_at(d)),
                )
            with scope("wait_pos"):
                arrived(pos, prows, S_PL, S_PR)
            with scope("build"):
                build()
        with scope(f"wait_window#k={k}"):
            arrived(windows[k], urows, S_FL + k, S_FR + k)
        with scope(f"near#k={k}"):
            apply_near(windows[k])
        if k < ITERS - 1:
            with scope(f"sums#k={k + 1}"):
                put_sums(k + 1, *near_state())
                share_sums(k + 1)
        if k == 0:
            with scope("lin"):
                drain(lin.at[pl.ds(0, ngrp - 1)], recv_sem.at[S_LIN])
                for t in range(4):
                    lint[t] = functools.reduce(jnp.add, [lin[j, t] for j in range(ngrp)])
        with scope(f"wait_far#k={k}"):
            drain(tables[k].at[pl.ds(0, ncell - 1)], recv_sem.at[S_TB + k])
        with scope(f"far#k={k}"):
            mu, q = new_state(*apply_far(k))
        if k < ITERS - 1:
            with scope(f"send#k={k + 1}"):
                put_state(k + 1, mu, q)
                share_state(k + 1)
            with scope(f"answer#k={k + 1}"):
                answer = far_answer()
        else:
            for a in range(3):
                for b in range(lb):
                    out_mu[a : a + 1, lanes(b)] = mu[a][b]
            for g in range(lg):
                out_q[g : g + 1] = q[g]

    def sent(ref, rows, sem_group, sem_left, sem_right):
        size = ngrp * rows
        drain(ref.at[pl.ds(0, (ngrp - 1) * rows)], send_sem.at[sem_group])

        @pl.when(cell < ncell - 1)
        def _():
            drain(ref.at[pl.ds(0, size)], send_sem.at[sem_right])

        @pl.when(cell > 0)
        def _():
            drain(ref.at[pl.ds(0, size)], send_sem.at[sem_left])

    sent(pos, prows, S_POS, S_PL, S_PR)
    drain(lin.at[pl.ds(0, ngrp - 1)], send_sem.at[S_LIN])
    for k in range(ITERS):
        drain(sa.at[pl.ds(0, ngrp - 1)], send_sem.at[S_SA + k])
        drain(tables[k].at[pl.ds(0, ncell - 1)], send_sem.at[S_TB + k])
        sent(windows[k], urows, S_W + k, S_FL + k, S_FR + k)


def body(
    ncell, ngrp,
    atom_sites, grid_points, dipole_guess, fixed_field, polarisability, base_charge, response,
    near_blocks, grid_blocks, source_blocks,
):
    lb, nb = near_blocks.shape
    nq = grid_blocks.shape[1]
    lg, nm = source_blocks.shape
    urows = 3 * lb + lg
    prows = 3 * lb + 3 * lg
    vmem = pl.BlockSpec(memory_space=pltpu.VMEM)
    tile = (BLOCK, BLOCK)
    window = pltpu.VMEM((3 * ngrp * urows, 1, BLOCK), F32)
    table = pltpu.VMEM((ncell, 1, BLOCK), F32)
    mu, q = pl.pallas_call(
        functools.partial(kernel, ncell, ngrp, lb, lg, nb, nq, nm),
        out_shape=(
            pltpu.VMEM((3, lb * BLOCK), F32),
            pltpu.VMEM((lg, BLOCK), F32),
        ),
        in_specs=[pl.BlockSpec(memory_space=pl.ANY)] * 10,
        out_specs=(vmem, vmem),
        scratch_shapes=[
            pltpu.SMEM(near_blocks.shape, jnp.int32),
            pltpu.SMEM(grid_blocks.shape, jnp.int32),
            pltpu.SMEM(source_blocks.shape, jnp.int32),
            pltpu.VMEM((3, lb * BLOCK), F32),
            pltpu.VMEM((3, lg * BLOCK), F32),
            pltpu.VMEM((3, lb * BLOCK), F32),
            pltpu.VMEM((3, lb * BLOCK), F32),
            pltpu.VMEM((lb, BLOCK), F32),
            pltpu.VMEM((lg, BLOCK), F32),
            pltpu.VMEM((lg, BLOCK), F32),
            pltpu.SMEM((lb * (nb + 1 + nq) + lg * nm,), jnp.int32),
            pltpu.SMEM((lb * (nb + 1 + nq) + lg * nm,), jnp.int32),
            window, window, window,
            pltpu.VMEM((3 * ngrp * prows, 1, BLOCK), F32),
            pltpu.VMEM((ITERS * ngrp, 1, BLOCK), F32),
            table, table, table,
            pltpu.VMEM(((lb + lg) * 3, *tile), F32),
            pltpu.VMEM((lb * (nb + 1) * 4, *tile), F32),
            pltpu.VMEM((lb * nq * 3, *tile), F32),
            pltpu.VMEM((lg * nm * 3, *tile), F32),
            pltpu.VMEM((lb * 9, ncell, BLOCK), F32),
            pltpu.VMEM((lg * 3, ncell, BLOCK), F32),
            pltpu.VMEM((14, *tile), F32),
            pltpu.VMEM((ngrp, 4, 8, BLOCK), F32),
            pltpu.VMEM((4, 8, BLOCK), F32),
            pltpu.VMEM((ncell, BLOCK), F32),
            pltpu.VMEM(((nb + 1) * 3 + nq, 8, BLOCK), F32),
            pltpu.VMEM((3 * lb + lg, *tile), F32),
            pltpu.VMEM((3 * lb + lg, 1, BLOCK), F32),
            pltpu.SemaphoreType.DMA((10,)),
            pltpu.SemaphoreType.DMA((19,)),
            pltpu.SemaphoreType.DMA((19,)),
            pltpu.SemaphoreType.REGULAR((3,)),
        ],
        compiler_params=pltpu.CompilerParams(
            collective_id=0, has_side_effects=True, vmem_limit_bytes=60 * 1024 * 1024
        ),
    )(
        near_blocks, grid_blocks, source_blocks,
        atom_sites, grid_points, dipole_guess, fixed_field,
        polarisability.reshape(lb, BLOCK), base_charge.reshape(lg, BLOCK),
        response.reshape(lg, BLOCK),
    )
    return mu, q.reshape(-1)


def solution(mesh):
    shared = P(None, ("cell", "grp"))
    flat = P(("cell", "grp"))
    rows = P(("cell", "grp"), None)
    return jax.shard_map(
        functools.partial(body, mesh.shape["cell"], mesh.shape["grp"]),
        mesh=mesh,
        in_specs=(shared, shared, shared, shared, flat, flat, flat, rows, rows, rows),
        out_specs=(shared, flat),
        check_vma=False,
    )
```

```python
import functools

import jax
import jax.numpy as jnp
from jax import lax
from jax.experimental import pallas as pl
from jax.experimental.pallas import tpu as pltpu
from jax.sharding import PartitionSpec as P

BLOCK = 128
ITERS = 3
CHUNK = 32
SOFT = 0.04
ROOT3 = 3.0**0.5
DIRECT_P = True
DIRECT_W = (True, True, True)
MESH = pl.DeviceIdType.MESH
F32 = jnp.float32


def copy_to(src, dst, send_sem, recv_sem, device):
    pltpu.make_async_remote_copy(
        src_ref=src,
        dst_ref=dst,
        send_sem=send_sem,
        recv_sem=recv_sem,
        device_id=device,
        device_id_type=MESH,
    ).start()


def drain(ref, sem):
    pltpu.make_async_copy(ref, ref, sem).wait()


def ring_order(size):
    return sorted(range(1, size), key=lambda d: -min(d, size - d))


def far_order(ncell):
    def hops(d):
        total = 0
        for c in range(ncell):
            a, b = c // 2, (c + d) % ncell // 2
            dz, dx = abs(a % 8 - b % 8), abs(a // 8 - b // 8)
            total += min(dz, 8 - dz) + min(dx, ncell // 16 - dx)
        return total

    return sorted(range(1, ncell), key=lambda d: (-hops(d), d))


def powers(dx, dy, dz):
    s = lax.rsqrt(dx * dx + dy * dy + dz * dz + SOFT)
    return s, s * s * s


def pair_tensor(dx, dy, dz, s3, s5):
    t = 3.0 * s5
    tx, ty, tz = t * dx, t * dy, t * dz
    return (tx * dx - s3, tx * dy, tx * dz, ty * dy - s3, ty * dz, tz * dz - s3)


def kernel(
    ncell, ngrp, lb, lg, nb, nq, nm,
    near_in, grid_in, source_in,
    sites_in, points_in, guess_in, fixed_in, pol_in, base_in, resp_in,
    out_mu, out_q,
    near_list, grid_list, source_list,
    sites, points, guess, fixed, pol, base, resp,
    urow, prow,
    w0, w1, w2, pos, sa, tb0, tb1, tb2,
    tgt, td, tc, tp, fd, fp, zst, lin, lint, tab, mub, accs, nf,
    local_sem, send_sem, recv_sem, hello,
):
    windows = (w0, w1, w2)
    tables = (tb0, tb1, tb2)
    cell = lax.axis_index("cell")
    grp = lax.axis_index("grp")
    urows = 3 * lb + lg
    prows = 3 * lb + 3 * lg
    slots = nb + 1
    own = ngrp + grp

    others = far_order(ncell)

    def cell_at(d):
        return (cell + d) & (ncell - 1)

    def group_at(d):
        return (grp + d) & (ngrp - 1)

    def signal(sem, to_cell, to_grp):
        pl.semaphore_signal(sem, inc=1, device_id=(to_cell, to_grp), device_id_type=MESH)

    beside = cell_at(2 * (cell & 1) - 1)
    partner = cell ^ 1
    line = cell & 14
    z_line = [(cell - line) + ((line + 2 * d) & 14) for d in ring_order(8)]
    x_line = [cell_at(16 * d) for d in range(1, ncell // 16)]
    barrier = pltpu.get_barrier_semaphore()
    with jax.named_scope("greet"):
        for d in ring_order(ngrp):
            signal(barrier, cell, group_at(d))
        for other in z_line + x_line + [beside, partner]:
            signal(barrier, other, grp)
    greeted = ngrp - 1 + len(z_line) + len(x_line) + 2
    loads = [
        pltpu.make_async_copy(src, dst, local_sem.at[n])
        for n, (src, dst) in enumerate(
            (
                (sites_in, sites), (points_in, points), (guess_in, guess), (base_in, base),
                (near_in, near_list), (grid_in, grid_list), (source_in, source_list),
                (fixed_in, fixed), (pol_in, pol), (resp_in, resp),
            )
        )
    ]
    for load in loads:
        load.start()
    for load in loads:
        load.wait()

    tiles = BLOCK // 8

    def tile(t):
        return pl.ds(8 * t, 8)

    def lanes(j):
        return pl.ds(j * BLOCK, BLOCK)

    zc = [cell.astype(F32) + 0.5, 0.5, 0.5]
    lane = lax.broadcasted_iota(jnp.int32, (1, BLOCK), 1)

    def put_sums(k, mu, q):
        sums = [functools.reduce(jnp.add, mu[a]) for a in range(3)]
        sums.append(functools.reduce(jnp.add, q))
        for a in range(3):
            moment = functools.reduce(jnp.add, [q[g] * offsets(a, g) for g in range(lg)])
            sums.append(moment + sums[a])
        row = jnp.zeros((1, BLOCK), F32)
        for n, total in enumerate(sums):
            row = jnp.where(lane == n, jnp.sum(total, axis=1, keepdims=True), row)
        sa[k * ngrp + grp] = row

    def put_state(k, mu, q):
        w = windows[k]
        for a in range(3):
            for b in range(lb):
                w[own * urows + a * lb + b] = mu[a][b]
        for g in range(lg):
            w[own * urows + 3 * lb + g] = q[g]

    def offsets(a, g):
        return points[a : a + 1, lanes(g)] - zc[a]

    for a in range(3):
        for b in range(lb):
            pos[own * prows + a * lb + b] = sites[a : a + 1, lanes(b)]
        for g in range(lg):
            pos[own * prows + 3 * lb + a * lg + g] = points[a : a + 1, lanes(g)]
    first = (
        [[guess[a : a + 1, lanes(b)] for b in range(lb)] for a in range(3)],
        [base[g : g + 1] for g in range(lg)],
    )
    put_sums(0, *first)
    put_state(0, *first)

    def atom_rows(n, w):
        at, b = lax.shift_right_logical(w, lb.bit_length() - 1), w & (lb - 1)
        urow[n] = at * urows + b
        prow[n] = at * prows + b

    def grid_rows(n, w):
        at = w // lg
        b = w - at * lg
        urow[n] = at * urows + 3 * lb + b
        prow[n] = at * prows + 3 * lb + b

    A_GRID = lb * slots
    A_SRC = A_GRID + lb * nq
    for b in range(lb):
        atom_rows(b * slots, own * lb + b)
        for s in range(nb):
            atom_rows(b * slots + 1 + s, near_list[b, s])
        for s in range(nq):
            grid_rows(A_GRID + b * nq + s, grid_list[b, s])
    for g in range(lg):
        for s in range(nm):
            atom_rows(A_SRC + g * nm + s, source_list[g, s])

    def clear(start):
        for w in windows:
            w[pl.ds(start * ngrp * urows, ngrp * urows)] = jnp.zeros(
                (ngrp * urows, 1, BLOCK), F32
            )
        pos[pl.ds(start * ngrp * prows, ngrp * prows)] = jnp.zeros((ngrp * prows, 1, BLOCK), F32)

    @pl.when(cell == 0)
    def _():
        clear(0)

    @pl.when(cell == ncell - 1)
    def _():
        clear(2)

    S_SA, S_W, S_FL, S_FR, S_TB = 0, 3, 6, 9, 12
    S_POS, S_PL, S_PR, S_LIN = 15, 16, 17, 18

    def share_group(ref, start, count, sem):
        part = ref.at[pl.ds(start, count)]
        for d in ring_order(ngrp):
            copy_to(part, part, send_sem.at[sem], recv_sem.at[sem], (cell, group_at(d)))

    def share_sums(k):
        share_group(sa, k * ngrp + grp, 1, S_SA + k)

    def share_direct(ref, rows, sem_group, sem_left, sem_right):
        part = ref.at[pl.ds(own * rows, rows)]
        left = ref.at[pl.ds(grp * rows, rows)]
        right = ref.at[pl.ds((2 * ngrp + grp) * rows, rows)]
        for d in ring_order(ngrp):
            copy_to(
                part, part, send_sem.at[sem_group], recv_sem.at[sem_group], (cell, group_at(d))
            )

        if ref is pos:
            pl.semaphore_wait(hello.at[0], 1)
        beyond = ring_order(ngrp) + [0]

        @pl.when(((cell & 1) == 1) & (cell < ncell - 1))
        def _():
            for d in beyond:
                copy_to(
                    part, left,
                    send_sem.at[sem_right], recv_sem.at[sem_right], (cell + 1, group_at(d)),
                )

        @pl.when(((cell & 1) == 0) & (cell > 0))
        def _():
            for d in beyond:
                copy_to(
                    part, right,
                    send_sem.at[sem_left], recv_sem.at[sem_left], (cell - 1, group_at(d)),
                )

    def forward_partner(ref, rows, sem_group, sem_left, sem_right):
        drain(ref.at[pl.ds(0, (ngrp - 1) * rows)], recv_sem.at[sem_group])
        size = ngrp * rows
        mine = ref.at[pl.ds(size, size)]

        @pl.when((cell & 1) == 0)
        def _():
            copy_to(
                mine, ref.at[pl.ds(0, size)],
                send_sem.at[sem_right], recv_sem.at[sem_right], (cell + 1, grp),
            )

        @pl.when((cell & 1) == 1)
        def _():
            copy_to(
                mine, ref.at[pl.ds(2 * size, size)],
                send_sem.at[sem_left], recv_sem.at[sem_left], (cell - 1, grp),
            )

    def share_state(k):
        if DIRECT_W[k]:
            share_direct(windows[k], urows, S_W + k, S_FL + k, S_FR + k)
        else:
            share_group(windows[k], own * urows, urows, S_W + k)

    def share_cell(k, answer):
        drain(sa.at[pl.ds(0, ngrp - 1)], recv_sem.at[S_SA + k])
        total = functools.reduce(jnp.add, [sa[k * ngrp + j] for j in range(ngrp)])
        if answer is not None:
            total = total + answer
        table = tables[k]
        table[cell] = total

        part = table.at[pl.ds(cell, 1)]
        for d in others:
            copy_to(
                part, part, send_sem.at[S_TB + k], recv_sem.at[S_TB + k], (cell_at(d), grp)
            )

    def forward(ref, rows, sem_group, sem_left, sem_right):
        drain(ref.at[pl.ds(0, (ngrp - 1) * rows)], recv_sem.at[sem_group])
        size = ngrp * rows
        mine = ref.at[pl.ds(size, size)]

        @pl.when(cell < ncell - 1)
        def _():
            copy_to(
                mine, ref.at[pl.ds(0, size)],
                send_sem.at[sem_right], recv_sem.at[sem_right], (cell + 1, grp),
            )

        @pl.when(cell > 0)
        def _():
            copy_to(
                mine, ref.at[pl.ds(2 * size, size)],
                send_sem.at[sem_left], recv_sem.at[sem_left], (cell - 1, grp),
            )

    def arrived(ref, rows, sem_left, sem_right):
        size = ngrp * rows

        @pl.when(cell > 0)
        def _():
            drain(ref.at[pl.ds(0, size)], recv_sem.at[sem_right])

        @pl.when(cell < ncell - 1)
        def _():
            drain(ref.at[pl.ds(2 * size, size)], recv_sem.at[sem_left])

    def wide(row):
        return jnp.broadcast_to(row, (8, BLOCK))

    def build():
        diagonal = lax.broadcasted_iota(jnp.int32, (8, BLOCK), 1) - lax.broadcasted_iota(
            jnp.int32, (8, BLOCK), 0
        )

        def deltas(j, t, rows):
            return [tgt[j * 3 + a, tile(t)] - rows[a] for a in range(3)]

        def dipole_slot(b, n, own_block):
            r = prow[n]
            rows = [wide(pos[r + a * lb]) for a in range(3)]
            for t in range(tiles):
                dx, dy, dz = deltas(b, t, rows)
                s1, s3 = powers(dx, dy, dz)
                w = ROOT3 * (s3 * lax.rsqrt(s1))
                if own_block:
                    s3 = jnp.where(diagonal == 8 * t, 0.0, s3)
                for i, v in enumerate((w * dx, w * dy, w * dz, s3)):
                    td[(n * tiles + t) * 4 + i] = v

        def charge_slot(ref, j, n, at, step):
            r = prow[n]
            rows = [wide(pos[r + a * step]) for a in range(3)]
            for t in range(tiles):
                dx, dy, dz = deltas(j, t, rows)
                _, s3 = powers(dx, dy, dz)
                for i, v in enumerate((dx, dy, dz)):
                    ref[(at * tiles + t) * 3 + i] = v * s3

        def atoms(b, carry):
            dipole_slot(b, b * slots, True)

            def some(i, c):
                for e in range(4):
                    dipole_slot(b, b * slots + 1 + 4 * i + e, False)
                return c

            lax.fori_loop(0, nb // 4, some, 0)

            for s in range(nq):
                charge_slot(tc, b, A_GRID + b * nq + s, b * nq + s, lg)
            return carry

        lax.fori_loop(0, lb, atoms, 0)
        forward_window(0)

        def grids(i, carry):
            g = i // (nm // 4)
            for e in range(4):
                at = 4 * i + e
                charge_slot(tp, lb + g, A_SRC + at, at, lb)
            return carry

        lax.fori_loop(0, lg * nm // 4, grids, 0)

    def reduce_rows(j):
        nf[j] = jnp.sum(jnp.transpose(accs[j]), axis=0, keepdims=True)

    def apply_own(w):
        def atoms(b, carry):
            m = [wide(w[own * urows + a * lb + b]) for a in range(3)]
            for t in range(tiles):
                vx, vy, vz, s3 = [td[(b * slots * tiles + t) * 4 + n] for n in range(4)]
                p = vx * m[0] + vy * m[1] + vz * m[2]
                for a, v in enumerate((vx, vy, vz)):
                    accs[b * 3 + a, tile(t)] = v * p - s3 * m[a]
            return carry

        lax.fori_loop(0, lb, atoms, 0)

    def apply_near(w):
        parts = CHUNK // 8

        def atoms(b, carry):
            for s in range(1, slots):
                r = urow[b * slots + s]
                for a in range(3):
                    mub[s * 3 + a] = wide(w[r + a * lb])
            for s in range(nq):
                mub[slots * 3 + s] = wide(w[urow[A_GRID + b * nq + s]])
            before = jnp.maximum(b - 1, 0)
            for c in range(BLOCK // CHUNK):
                rows = [tile(c * parts + i) for i in range(parts)]
                acc = [[accs[b * 3 + a, row] for row in rows] for a in range(3)]
                for s in range(1, slots):
                    m = [mub[s * 3 + a] for a in range(3)]
                    at = (b * slots + s) * tiles + c * parts
                    for i in range(parts):
                        vx, vy, vz, s3 = [td[(at + i) * 4 + n] for n in range(4)]
                        p = vx * m[0] + vy * m[1] + vz * m[2]
                        for a, v in enumerate((vx, vy, vz)):
                            acc[a][i] = acc[a][i] + (v * p - s3 * m[a])
                for s in range(nq):
                    q = mub[slots * 3 + s]
                    for i in range(parts):
                        for a in range(3):
                            at = (b * nq + s) * tiles + c * parts + i
                            acc[a][i] = acc[a][i] + tc[at * 3 + a] * q
                for a in range(3):
                    for i in range(parts):
                        accs[b * 3 + a, rows[i]] = acc[a][i]
                if c < 3:
                    reduce_rows(before * 3 + c)
            return carry

        lax.fori_loop(0, lb, atoms, 0)

        def grids(g, carry):
            for s in range(nm):
                r = urow[A_SRC + g * nm + s]
                for a in range(3):
                    mub[s * 3 + a] = wide(w[r + a * lb])
            acc = [jnp.zeros((8, BLOCK), F32) for _ in range(tiles)]
            for s in range(nm):
                m = [mub[s * 3 + a] for a in range(3)]
                at = (g * nm + s) * tiles
                for i in range(tiles):
                    acc[i] = acc[i] + (
                        tp[(at + i) * 3] * m[0] + tp[(at + i) * 3 + 1] * m[1]
                        + tp[(at + i) * 3 + 2] * m[2]
                    )
            for i in range(tiles):
                accs[3 * lb + g, tile(i)] = acc[i]
            reduce_rows(3 * lb - 3 + g)
            return carry

        lax.fori_loop(0, lg, grids, 0)
        for g in range(lg):
            reduce_rows(3 * lb + g)

    def apply_far(k):
        table = tables[k]
        acc = [[jnp.zeros((8, BLOCK), F32) for _ in range(lb)] for _ in range(3)]
        pot = [jnp.zeros((8, BLOCK), F32) for _ in range(lg)]
        for c in range(ncell):
            tab[c : c + 1] = table[c]
        for c8 in range(ncell // 8):
            row = tile(c8)
            rows = tab[row]
            px, py, pz, q, mx, my, mz = [
                jnp.broadcast_to(rows[:, n : n + 1], (8, BLOCK)) for n in range(7)
            ]
            for b in range(lb):
                xx, xy, xz, yy, yz, zz, cx, cy, cz = [fd[b * 9 + n, row] for n in range(9)]
                acc[0][b] = acc[0][b] + ((xx * mx + xy * my) + (xz * mz + cx * q))
                acc[1][b] = acc[1][b] + ((xy * mx + yy * my) + (yz * mz + cy * q))
                acc[2][b] = acc[2][b] + ((xz * mx + yz * my) + (zz * mz + cz * q))
            for g in range(lg):
                pot[g] = pot[g] + (
                    fp[g * 3, row] * px + fp[g * 3 + 1, row] * py + fp[g * 3 + 2, row] * pz
                )
        field = [
            [jnp.sum(acc[a][b], axis=0, keepdims=True) + nf[b * 3 + a] for b in range(lb)]
            for a in range(3)
        ]
        potential = [
            jnp.sum(pot[g], axis=0, keepdims=True) + nf[3 * lb + g] for g in range(lg)
        ]
        return field, potential

    def far_answer():
        rows = tab[...]
        flat = jnp.transpose(jnp.concatenate([rows, rows], axis=0))
        px, py, pz, q, mx, my, mz = [flat[n : n + 1] for n in range(7)]
        left = lane < ncell
        halves = (
            jnp.where(left, mx, my), jnp.where(left, mz, q),
            jnp.where(left, px, py), jnp.where(left, pz, 0.0),
        )
        total = functools.reduce(jnp.add, [lint[t] * halves[t] for t in range(4)])
        total = jnp.sum(total, axis=1, keepdims=True)
        lanes8 = lax.broadcasted_iota(jnp.int32, (8, BLOCK), 1)
        return jnp.sum(jnp.where(lanes8 == cells8, total, 0.0), axis=0, keepdims=True)

    def near_state():
        none = [[nf[b * 3 + a] for b in range(lb)] for a in range(3)]
        return new_state(none, [nf[3 * lb + g] for g in range(lg)])

    def new_state(field, potential):
        mu = [
            [pol[b : b + 1] * (fixed[a : a + 1, lanes(b)] + field[a][b]) for b in range(lb)]
            for a in range(3)
        ]
        q = [base[g : g + 1] - resp[g : g + 1] * potential[g] for g in range(lg)]
        return mu, q

    scope = jax.named_scope
    with scope("barrier"):
        pl.semaphore_wait(barrier, greeted)
    signal(hello.at[0], beside, grp)
    for other in z_line:
        signal(hello.at[1], other, grp)
    with scope("send0"):
        share_sums(0)
        if DIRECT_P:
            share_direct(pos, prows, S_POS, S_PL, S_PR)
        else:
            share_group(pos, own * prows, prows, S_POS)
    for a in range(3):
        for b in range(lb):
            tgt[b * 3 + a] = jnp.transpose(
                jnp.broadcast_to(sites[a : a + 1, lanes(b)], (BLOCK, BLOCK))
            )
        for g in range(lg):
            tgt[(lb + g) * 3 + a] = jnp.transpose(
                jnp.broadcast_to(points[a : a + 1, lanes(g)], (BLOCK, BLOCK))
            )

    cells8 = lax.broadcasted_iota(jnp.int32, (8, BLOCK), 0)

    def far_rows(ref, j, c8):
        number = cells8 + c8 * 8
        dx = ref[0:1, lanes(j)] - (number.astype(F32) + 0.5)
        dy = ref[1:2, lanes(j)] - 0.5 + jnp.zeros_like(dx)
        dz = ref[2:3, lanes(j)] - 0.5 + jnp.zeros_like(dx)
        keep = jnp.abs(number - cell) >= 2
        s1, s3 = powers(dx, dy, dz)
        s3 = jnp.where(keep, s3, 0.0)
        return dx, dy, dz, s3, s3 * s1 * s1

    def far_build(c8, carry):
        row = pl.ds(pl.multiple_of(c8 * 8, 8), 8)
        low = pl.ds(pl.multiple_of(ncell + c8 * 8, 8), 8)
        answer = [jnp.zeros((8, BLOCK), F32) for _ in range(9)]
        for b in range(lb):
            dx, dy, dz, s3, s5 = far_rows(sites, b, c8)
            values = (*pair_tensor(dx, dy, dz, s3, s5), dx * s3, dy * s3, dz * s3)
            for n, v in enumerate(values):
                fd[b * 9 + n, row] = v
                answer[n] = answer[n] + v * pol[b : b + 1]
        charge = [[jnp.zeros((8, BLOCK), F32) for _ in range(3)] for _ in range(4)]
        for g in range(lg):
            dx, dy, dz, s3, s5 = far_rows(points, g, c8)
            for n, v in enumerate((dx, dy, dz)):
                fp[g * 3 + n, row] = v * s3
                change = v * s3 * resp[g : g + 1]
                charge[0][n] = charge[0][n] - change
                for a in range(3):
                    charge[1 + a][n] = charge[1 + a][n] - change * offsets(a, g)
        xx, xy, xz, yy, yz, zz, cx, cy, cz = answer
        halves = [(xx, xy), (xy, yy), (xz, yz), (xz, cx), (yz, cy), (zz, cz)]
        halves += [(c[0], c[1]) for c in charge]
        halves += [(c[2], jnp.zeros((8, BLOCK), F32)) for c in charge]
        for n, (top, bottom) in enumerate(halves):
            zst[n, row] = top
            zst[n, low] = bottom
        return carry

    with jax.named_scope("far_build"):
        lax.fori_loop(0, ncell // 8, far_build, 0)
        places = [
            [(a, a) for a in range(3)] + [(4 + a, a) for a in range(3)],
            [(a, 3 + a) for a in range(3)] + [(4 + a, 3 + a) for a in range(3)],
            [(3 + a, 6 + a) for a in range(4)],
            [(3 + a, 10 + a) for a in range(4)],
        ]
        flat = [jnp.sum(jnp.transpose(zst[n]), axis=0, keepdims=True) for n in range(14)]
        for t in range(4):
            value = jnp.zeros((8, BLOCK), F32)
            for at, n in places[t]:
                value = jnp.where(cells8 == at, flat[n], value)
            lin[grp, t] = value

    share_state(0)
    with scope("hello"):
        pl.semaphore_wait(hello.at[1], len(z_line))
        signal(hello.at[2], partner, grp)
        pl.semaphore_wait(hello.at[2], 1)
    def sent(ref, rows, sem_group, sem_left, sem_right):
        size = ngrp * rows
        drain(ref.at[pl.ds(0, (ngrp - 1) * rows)], send_sem.at[sem_group])

        @pl.when(cell < ncell - 1)
        def _():
            drain(ref.at[pl.ds(0, size)], send_sem.at[sem_right])

        @pl.when(cell > 0)
        def _():
            drain(ref.at[pl.ds(0, size)], send_sem.at[sem_left])

    def sent_all(k):
        if k == 0:
            sent(pos, prows, S_POS, S_PL, S_PR)
            drain(lin.at[pl.ds(0, ngrp - 1)], send_sem.at[S_LIN])
        drain(sa.at[pl.ds(0, ngrp - 1)], send_sem.at[S_SA + k])
        drain(tables[k].at[pl.ds(0, ncell - 1)], send_sem.at[S_TB + k])
        sent(windows[k], urows, S_W + k, S_FL + k, S_FR + k)

    def forward_window(k):
        (forward_partner if DIRECT_W[k] else forward)(
            windows[k], urows, S_W + k, S_FL + k, S_FR + k
        )

    answer = None
    for k in range(ITERS):
        with scope(f"share_cell#k={k}"):
            share_cell(k, answer)
        with scope(f"forward#k={k}"):
            if k == 0:
                (forward_partner if DIRECT_P else forward)(pos, prows, S_POS, S_PL, S_PR)
            if k > 0:
                forward_window(k)
                sent_all(k - 1)
        if k == 0:
            for d in ring_order(ngrp):
                copy_to(
                    lin.at[grp], lin.at[grp], send_sem.at[S_LIN], recv_sem.at[S_LIN],
                    (cell, group_at(d)),
                )
            with scope("wait_pos"):
                arrived(pos, prows, S_PL, S_PR)
            with scope("build"):
                build()
        with scope(f"own#k={k}"):
            apply_own(windows[k])
        with scope(f"wait_window#k={k}"):
            arrived(windows[k], urows, S_FL + k, S_FR + k)
        with scope(f"near#k={k}"):
            apply_near(windows[k])
        if k < ITERS - 1:
            with scope(f"sums#k={k + 1}"):
                put_sums(k + 1, *near_state())
                share_sums(k + 1)
        if k == 0:
            with scope("lin"):
                drain(lin.at[pl.ds(0, ngrp - 1)], recv_sem.at[S_LIN])
                for t in range(4):
                    lint[t] = functools.reduce(jnp.add, [lin[j, t] for j in range(ngrp)])
        with scope(f"wait_far#k={k}"):
            drain(tables[k].at[pl.ds(0, ncell - 1)], recv_sem.at[S_TB + k])
        with scope(f"far#k={k}"):
            mu, q = new_state(*apply_far(k))
        if k < ITERS - 1:
            with scope(f"send#k={k + 1}"):
                put_state(k + 1, mu, q)
                share_state(k + 1)
            with scope(f"answer#k={k + 1}"):
                answer = far_answer()
        else:
            for a in range(3):
                for b in range(lb):
                    out_mu[a : a + 1, lanes(b)] = mu[a][b]
            for g in range(lg):
                out_q[g : g + 1] = q[g]

    sent_all(ITERS - 1)


def body(
    ncell, ngrp,
    atom_sites, grid_points, dipole_guess, fixed_field, polarisability, base_charge, response,
    near_blocks, grid_blocks, source_blocks,
):
    lb, nb = near_blocks.shape
    nq = grid_blocks.shape[1]
    lg, nm = source_blocks.shape
    urows = 3 * lb + lg
    prows = 3 * lb + 3 * lg
    vmem = pl.BlockSpec(memory_space=pltpu.VMEM)
    tile = (BLOCK, BLOCK)
    window = pltpu.VMEM((3 * ngrp * urows, 1, BLOCK), F32)
    table = pltpu.VMEM((ncell, 1, BLOCK), F32)
    mu, q = pl.pallas_call(
        functools.partial(kernel, ncell, ngrp, lb, lg, nb, nq, nm),
        out_shape=(
            pltpu.VMEM((3, lb * BLOCK), F32),
            pltpu.VMEM((lg, BLOCK), F32),
        ),
        in_specs=[pl.BlockSpec(memory_space=pl.ANY)] * 10,
        out_specs=(vmem, vmem),
        scratch_shapes=[
            pltpu.SMEM(near_blocks.shape, jnp.int32),
            pltpu.SMEM(grid_blocks.shape, jnp.int32),
            pltpu.SMEM(source_blocks.shape, jnp.int32),
            pltpu.VMEM((3, lb * BLOCK), F32),
            pltpu.VMEM((3, lg * BLOCK), F32),
            pltpu.VMEM((3, lb * BLOCK), F32),
            pltpu.VMEM((3, lb * BLOCK), F32),
            pltpu.VMEM((lb, BLOCK), F32),
            pltpu.VMEM((lg, BLOCK), F32),
            pltpu.VMEM((lg, BLOCK), F32),
            pltpu.SMEM((lb * (nb + 1 + nq) + lg * nm,), jnp.int32),
            pltpu.SMEM((lb * (nb + 1 + nq) + lg * nm,), jnp.int32),
            window, window, window,
            pltpu.VMEM((3 * ngrp * prows, 1, BLOCK), F32),
            pltpu.VMEM((ITERS * ngrp, 1, BLOCK), F32),
            table, table, table,
            pltpu.VMEM(((lb + lg) * 3, *tile), F32),
            pltpu.VMEM((lb * (nb + 1) * 64, 8, BLOCK), F32),
            pltpu.VMEM((lb * nq * 48, 8, BLOCK), F32),
            pltpu.VMEM((lg * nm * 48, 8, BLOCK), F32),
            pltpu.VMEM((lb * 9, ncell, BLOCK), F32),
            pltpu.VMEM((lg * 3, ncell, BLOCK), F32),
            pltpu.VMEM((14, *tile), F32),
            pltpu.VMEM((ngrp, 4, 8, BLOCK), F32),
            pltpu.VMEM((4, 8, BLOCK), F32),
            pltpu.VMEM((ncell, BLOCK), F32),
            pltpu.VMEM(((nb + 1) * 3 + nq, 8, BLOCK), F32),
            pltpu.VMEM((3 * lb + lg, *tile), F32),
            pltpu.VMEM((3 * lb + lg, 1, BLOCK), F32),
            pltpu.SemaphoreType.DMA((10,)),
            pltpu.SemaphoreType.DMA((19,)),
            pltpu.SemaphoreType.DMA((19,)),
            pltpu.SemaphoreType.REGULAR((3,)),
        ],
        compiler_params=pltpu.CompilerParams(
            collective_id=0, has_side_effects=True, vmem_limit_bytes=60 * 1024 * 1024
        ),
    )(
        near_blocks, grid_blocks, source_blocks,
        atom_sites, grid_points, dipole_guess, fixed_field,
        polarisability.reshape(lb, BLOCK), base_charge.reshape(lg, BLOCK),
        response.reshape(lg, BLOCK),
    )
    return mu, q.reshape(-1)


def solution(mesh):
    shared = P(None, ("cell", "grp"))
    flat = P(("cell", "grp"))
    rows = P(("cell", "grp"), None)
    return jax.shard_map(
        functools.partial(body, mesh.shape["cell"], mesh.shape["grp"]),
        mesh=mesh,
        in_specs=(shared, shared, shared, shared, flat, flat, flat, rows, rows, rows),
        out_specs=(shared, flat),
        check_vma=False,
    )
```

```python
import functools

import jax
import jax.numpy as jnp
from jax import lax
from jax.experimental import pallas as pl
from jax.experimental.pallas import tpu as pltpu
from jax.sharding import PartitionSpec as P

BLOCK = 128
ITERS = 3
CHUNK = 32
SOFT = 0.04
ROOT3 = 3.0**0.5
DIRECT_P = True
DIRECT_W = (True, True, True)
MESH = pl.DeviceIdType.MESH
F32 = jnp.float32


def copy_to(src, dst, send_sem, recv_sem, device):
    pltpu.make_async_remote_copy(
        src_ref=src,
        dst_ref=dst,
        send_sem=send_sem,
        recv_sem=recv_sem,
        device_id=device,
        device_id_type=MESH,
    ).start()


def drain(ref, sem):
    pltpu.make_async_copy(ref, ref, sem).wait()


def ring_order(size):
    return sorted(range(1, size), key=lambda d: -min(d, size - d))


def far_order(ncell):
    def hops(d):
        total = 0
        for c in range(ncell):
            a, b = c // 2, (c + d) % ncell // 2
            dz, dx = abs(a % 8 - b % 8), abs(a // 8 - b // 8)
            total += min(dz, 8 - dz) + min(dx, ncell // 16 - dx)
        return total

    return sorted(range(1, ncell), key=lambda d: (-hops(d), d))


def powers(dx, dy, dz):
    s = lax.rsqrt(dx * dx + dy * dy + dz * dz + SOFT)
    return s, s * s * s


def pair_tensor(dx, dy, dz, s3, s5):
    t = 3.0 * s5
    tx, ty, tz = t * dx, t * dy, t * dz
    return (tx * dx - s3, tx * dy, tx * dz, ty * dy - s3, ty * dz, tz * dz - s3)


def kernel(
    ncell, ngrp, lb, lg, nb, nq, nm,
    near_in, grid_in, source_in,
    sites_in, points_in, guess_in, fixed_in, pol_in, base_in, resp_in,
    out_mu, out_q,
    near_list, grid_list, source_list,
    sites, points, guess, fixed, pol, base, resp,
    urow, prow,
    w0, w1, w2, pos, sa, tb0, tb1, tb2,
    tgt, td, tc, tp, fd, fp, zst, lin, lint, tab, mus, mub, accs, nf,
    local_sem, send_sem, recv_sem, hello,
):
    windows = (w0, w1, w2)
    tables = (tb0, tb1, tb2)
    cell = lax.axis_index("cell")
    grp = lax.axis_index("grp")
    urows = 3 * lb + lg
    prows = 3 * lb + 3 * lg
    slots = nb + 1
    own = ngrp + grp

    others = far_order(ncell)

    def cell_at(d):
        return (cell + d) & (ncell - 1)

    def group_at(d):
        return (grp + d) & (ngrp - 1)

    def signal(sem, to_cell, to_grp):
        pl.semaphore_signal(sem, inc=1, device_id=(to_cell, to_grp), device_id_type=MESH)

    beside = cell_at(2 * (cell & 1) - 1)
    partner = cell ^ 1
    line = cell & 14
    z_line = [(cell - line) + ((line + 2 * d) & 14) for d in ring_order(8)]
    x_line = [cell_at(16 * d) for d in range(1, ncell // 16)]
    barrier = pltpu.get_barrier_semaphore()
    with jax.named_scope("greet"):
        for d in ring_order(ngrp):
            signal(barrier, cell, group_at(d))
        for other in z_line + x_line + [beside, partner]:
            signal(barrier, other, grp)
    greeted = ngrp - 1 + len(z_line) + len(x_line) + 2
    loads = [
        pltpu.make_async_copy(src, dst, local_sem.at[n])
        for n, (src, dst) in enumerate(
            (
                (sites_in, sites), (points_in, points), (guess_in, guess), (base_in, base),
                (near_in, near_list), (grid_in, grid_list), (source_in, source_list),
                (fixed_in, fixed), (pol_in, pol), (resp_in, resp),
            )
        )
    ]
    for load in loads:
        load.start()
    for load in loads:
        load.wait()

    tiles = BLOCK // 8

    def tile(t):
        return pl.ds(8 * t, 8)

    def lanes(j):
        return pl.ds(j * BLOCK, BLOCK)

    zc = [cell.astype(F32) + 0.5, 0.5, 0.5]
    lane = lax.broadcasted_iota(jnp.int32, (1, BLOCK), 1)

    def put_sums(k, mu, q):
        sums = [functools.reduce(jnp.add, mu[a]) for a in range(3)]
        sums.append(functools.reduce(jnp.add, q))
        for a in range(3):
            moment = functools.reduce(jnp.add, [q[g] * offsets(a, g) for g in range(lg)])
            sums.append(moment + sums[a])
        row = jnp.zeros((1, BLOCK), F32)
        for n, total in enumerate(sums):
            row = jnp.where(lane == n, jnp.sum(total, axis=1, keepdims=True), row)
        sa[k * ngrp + grp] = row

    def put_state(k, mu, q):
        w = windows[k]
        for a in range(3):
            for b in range(lb):
                w[own * urows + a * lb + b] = mu[a][b]
        for g in range(lg):
            w[own * urows + 3 * lb + g] = q[g]

    def offsets(a, g):
        return points[a : a + 1, lanes(g)] - zc[a]

    for a in range(3):
        for b in range(lb):
            pos[own * prows + a * lb + b] = sites[a : a + 1, lanes(b)]
        for g in range(lg):
            pos[own * prows + 3 * lb + a * lg + g] = points[a : a + 1, lanes(g)]
    first = (
        [[guess[a : a + 1, lanes(b)] for b in range(lb)] for a in range(3)],
        [base[g : g + 1] for g in range(lg)],
    )
    put_sums(0, *first)
    put_state(0, *first)

    def atom_rows(n, w):
        at, b = lax.shift_right_logical(w, lb.bit_length() - 1), w & (lb - 1)
        urow[n] = at * urows + b
        prow[n] = at * prows + b

    def grid_rows(n, w):
        at = w // lg
        b = w - at * lg
        urow[n] = at * urows + 3 * lb + b
        prow[n] = at * prows + 3 * lb + b

    A_GRID = lb * slots
    A_SRC = A_GRID + lb * nq
    for b in range(lb):
        atom_rows(b * slots, own * lb + b)
        for s in range(nb):
            atom_rows(b * slots + 1 + s, near_list[b, s])
        for s in range(nq):
            grid_rows(A_GRID + b * nq + s, grid_list[b, s])
    for g in range(lg):
        for s in range(nm):
            atom_rows(A_SRC + g * nm + s, source_list[g, s])

    def clear(start):
        for w in windows:
            w[pl.ds(start * ngrp * urows, ngrp * urows)] = jnp.zeros(
                (ngrp * urows, 1, BLOCK), F32
            )
        pos[pl.ds(start * ngrp * prows, ngrp * prows)] = jnp.zeros((ngrp * prows, 1, BLOCK), F32)

    @pl.when(cell == 0)
    def _():
        clear(0)

    @pl.when(cell == ncell - 1)
    def _():
        clear(2)

    S_SA, S_W, S_FL, S_FR, S_TB = 0, 3, 6, 9, 12
    S_POS, S_PL, S_PR, S_LIN = 15, 16, 17, 18

    def share_group(ref, start, count, sem):
        part = ref.at[pl.ds(start, count)]
        for d in ring_order(ngrp):
            copy_to(part, part, send_sem.at[sem], recv_sem.at[sem], (cell, group_at(d)))

    def share_sums(k):
        share_group(sa, k * ngrp + grp, 1, S_SA + k)

    def share_direct(ref, rows, sem_group, sem_left, sem_right):
        part = ref.at[pl.ds(own * rows, rows)]
        left = ref.at[pl.ds(grp * rows, rows)]
        right = ref.at[pl.ds((2 * ngrp + grp) * rows, rows)]
        for d in ring_order(ngrp):
            copy_to(
                part, part, send_sem.at[sem_group], recv_sem.at[sem_group], (cell, group_at(d))
            )

        if ref is pos:
            pl.semaphore_wait(hello.at[0], 1)
        beyond = ring_order(ngrp) + [0]

        @pl.when(((cell & 1) == 1) & (cell < ncell - 1))
        def _():
            for d in beyond:
                copy_to(
                    part, left,
                    send_sem.at[sem_right], recv_sem.at[sem_right], (cell + 1, group_at(d)),
                )

        @pl.when(((cell & 1) == 0) & (cell > 0))
        def _():
            for d in beyond:
                copy_to(
                    part, right,
                    send_sem.at[sem_left], recv_sem.at[sem_left], (cell - 1, group_at(d)),
                )

    def forward_partner(ref, rows, sem_group, sem_left, sem_right):
        drain(ref.at[pl.ds(0, (ngrp - 1) * rows)], recv_sem.at[sem_group])
        size = ngrp * rows
        mine = ref.at[pl.ds(size, size)]

        @pl.when((cell & 1) == 0)
        def _():
            copy_to(
                mine, ref.at[pl.ds(0, size)],
                send_sem.at[sem_right], recv_sem.at[sem_right], (cell + 1, grp),
            )

        @pl.when((cell & 1) == 1)
        def _():
            copy_to(
                mine, ref.at[pl.ds(2 * size, size)],
                send_sem.at[sem_left], recv_sem.at[sem_left], (cell - 1, grp),
            )

    def share_state(k):
        if DIRECT_W[k]:
            share_direct(windows[k], urows, S_W + k, S_FL + k, S_FR + k)
        else:
            share_group(windows[k], own * urows, urows, S_W + k)

    def share_cell(k, answer):
        drain(sa.at[pl.ds(0, ngrp - 1)], recv_sem.at[S_SA + k])
        total = functools.reduce(jnp.add, [sa[k * ngrp + j] for j in range(ngrp)])
        if answer is not None:
            total = total + answer
        table = tables[k]
        table[cell] = total

        part = table.at[pl.ds(cell, 1)]
        for d in others:
            copy_to(
                part, part, send_sem.at[S_TB + k], recv_sem.at[S_TB + k], (cell_at(d), grp)
            )

    def forward(ref, rows, sem_group, sem_left, sem_right):
        drain(ref.at[pl.ds(0, (ngrp - 1) * rows)], recv_sem.at[sem_group])
        size = ngrp * rows
        mine = ref.at[pl.ds(size, size)]

        @pl.when(cell < ncell - 1)
        def _():
            copy_to(
                mine, ref.at[pl.ds(0, size)],
                send_sem.at[sem_right], recv_sem.at[sem_right], (cell + 1, grp),
            )

        @pl.when(cell > 0)
        def _():
            copy_to(
                mine, ref.at[pl.ds(2 * size, size)],
                send_sem.at[sem_left], recv_sem.at[sem_left], (cell - 1, grp),
            )

    def arrived(ref, rows, sem_left, sem_right):
        size = ngrp * rows

        @pl.when(cell > 0)
        def _():
            drain(ref.at[pl.ds(0, size)], recv_sem.at[sem_right])

        @pl.when(cell < ncell - 1)
        def _():
            drain(ref.at[pl.ds(2 * size, size)], recv_sem.at[sem_left])

    def wide(row):
        return jnp.broadcast_to(row, (8, BLOCK))

    def build():
        diagonal = lax.broadcasted_iota(jnp.int32, (8, BLOCK), 1) - lax.broadcasted_iota(
            jnp.int32, (8, BLOCK), 0
        )

        def deltas(j, t, rows):
            return [tgt[j * 3 + a, tile(t)] - rows[a] for a in range(3)]

        def dipole_slot(b, n, own_block):
            r = prow[n]
            rows = [wide(pos[r + a * lb]) for a in range(3)]
            for t in range(tiles):
                dx, dy, dz = deltas(b, t, rows)
                s1, s3 = powers(dx, dy, dz)
                w = ROOT3 * (s3 * lax.rsqrt(s1))
                if own_block:
                    s3 = jnp.where(diagonal == 8 * t, 0.0, s3)
                for i, v in enumerate((w * dx, w * dy, w * dz, s3)):
                    td[(n * tiles + t) * 4 + i] = v

        def charge_slot(ref, j, n, at, step):
            r = prow[n]
            rows = [wide(pos[r + a * step]) for a in range(3)]
            for t in range(tiles):
                dx, dy, dz = deltas(j, t, rows)
                _, s3 = powers(dx, dy, dz)
                for i, v in enumerate((dx, dy, dz)):
                    ref[(at * tiles + t) * 3 + i] = v * s3

        def atoms(b, carry):
            dipole_slot(b, b * slots, True)

            def some(i, c):
                for e in range(4):
                    dipole_slot(b, b * slots + 1 + 4 * i + e, False)
                return c

            lax.fori_loop(0, nb // 4, some, 0)

            for s in range(nq):
                charge_slot(tc, b, A_GRID + b * nq + s, b * nq + s, lg)
            return carry

        lax.fori_loop(0, lb, atoms, 0)
        forward_window(0)

        def grids(i, carry):
            g = i // (nm // 4)
            for e in range(4):
                at = 4 * i + e
                charge_slot(tp, lb + g, A_SRC + at, at, lb)
            return carry

        lax.fori_loop(0, lg * nm // 4, grids, 0)

    def reduce_rows(j):
        nf[j] = jnp.sum(jnp.transpose(accs[j]), axis=0, keepdims=True)

    def apply_own(w):
        def atoms(b, carry):
            m = [wide(w[own * urows + a * lb + b]) for a in range(3)]
            for t in range(tiles):
                vx, vy, vz, s3 = [td[(b * slots * tiles + t) * 4 + n] for n in range(4)]
                p = vx * m[0] + vy * m[1] + vz * m[2]
                for a, v in enumerate((vx, vy, vz)):
                    accs[b * 3 + a, tile(t)] = v * p - s3 * m[a]
            return carry

        lax.fori_loop(0, lb, atoms, 0)

    def apply_near(w):
        parts = CHUNK // 8

        def pick_grids(n, carry):
            r = urow[A_SRC + n]
            for a in range(3):
                mus[n * 3 + a] = wide(w[r + a * lb])
            return carry

        lax.fori_loop(0, lg * nm, pick_grids, 0, unroll=True)

        def grid_part(g, c):
            acc = [jnp.zeros((8, BLOCK), F32) for _ in range(parts)]
            for s in range(nm):
                m = [mus[(g * nm + s) * 3 + a] for a in range(3)]
                at = (g * nm + s) * tiles + c * parts
                for i in range(parts):
                    acc[i] = acc[i] + (
                        tp[(at + i) * 3] * m[0] + tp[(at + i) * 3 + 1] * m[1]
                        + tp[(at + i) * 3 + 2] * m[2]
                    )
            for i in range(parts):
                row = pl.ds(pl.multiple_of(c * CHUNK + 8 * i, 8), 8)
                accs[3 * lb + g, row] = acc[i]

        def atoms(b, carry):
            for s in range(1, slots):
                r = urow[b * slots + s]
                for a in range(3):
                    mub[s * 3 + a] = wide(w[r + a * lb])
            for s in range(nq):
                mub[slots * 3 + s] = wide(w[urow[A_GRID + b * nq + s]])
            before = jnp.maximum(b - 1, 0)
            for c in range(BLOCK // CHUNK):
                rows = [tile(c * parts + i) for i in range(parts)]
                acc = [[accs[b * 3 + a, row] for row in rows] for a in range(3)]
                for s in range(1, slots):
                    m = [mub[s * 3 + a] for a in range(3)]
                    at = (b * slots + s) * tiles + c * parts
                    for i in range(parts):
                        vx, vy, vz, s3 = [td[(at + i) * 4 + n] for n in range(4)]
                        p = vx * m[0] + vy * m[1] + vz * m[2]
                        for a, v in enumerate((vx, vy, vz)):
                            acc[a][i] = acc[a][i] + (v * p - s3 * m[a])
                for s in range(nq):
                    q = mub[slots * 3 + s]
                    for i in range(parts):
                        for a in range(3):
                            at = (b * nq + s) * tiles + c * parts + i
                            acc[a][i] = acc[a][i] + tc[at * 3 + a] * q
                for a in range(3):
                    for i in range(parts):
                        accs[b * 3 + a, rows[i]] = acc[a][i]
                if c < 3:
                    reduce_rows(before * 3 + c)
                if c < lg:
                    grid_part(c, b)
            return carry

        lax.fori_loop(0, lb, atoms, 0)

        for n in range(3):
            reduce_rows(3 * (lb - 1) + n)
        for g in range(lg):
            reduce_rows(3 * lb + g)

    def apply_far(k):
        table = tables[k]
        acc = [[jnp.zeros((8, BLOCK), F32) for _ in range(lb)] for _ in range(3)]
        pot = [jnp.zeros((8, BLOCK), F32) for _ in range(lg)]
        for c in range(ncell):
            tab[c : c + 1] = table[c]
        for c8 in range(ncell // 8):
            row = tile(c8)
            rows = tab[row]
            px, py, pz, q, mx, my, mz = [
                jnp.broadcast_to(rows[:, n : n + 1], (8, BLOCK)) for n in range(7)
            ]
            for b in range(lb):
                xx, xy, xz, yy, yz, zz, cx, cy, cz = [fd[b * 9 + n, row] for n in range(9)]
                acc[0][b] = acc[0][b] + ((xx * mx + xy * my) + (xz * mz + cx * q))
                acc[1][b] = acc[1][b] + ((xy * mx + yy * my) + (yz * mz + cy * q))
                acc[2][b] = acc[2][b] + ((xz * mx + yz * my) + (zz * mz + cz * q))
            for g in range(lg):
                pot[g] = pot[g] + (
                    fp[g * 3, row] * px + fp[g * 3 + 1, row] * py + fp[g * 3 + 2, row] * pz
                )
        field = [
            [jnp.sum(acc[a][b], axis=0, keepdims=True) + nf[b * 3 + a] for b in range(lb)]
            for a in range(3)
        ]
        potential = [
            jnp.sum(pot[g], axis=0, keepdims=True) + nf[3 * lb + g] for g in range(lg)
        ]
        return field, potential

    def far_answer():
        rows = tab[...]
        flat = jnp.transpose(jnp.concatenate([rows, rows], axis=0))
        px, py, pz, q, mx, my, mz = [flat[n : n + 1] for n in range(7)]
        left = lane < ncell
        halves = (
            jnp.where(left, mx, my), jnp.where(left, mz, q),
            jnp.where(left, px, py), jnp.where(left, pz, 0.0),
        )
        total = functools.reduce(jnp.add, [lint[t] * halves[t] for t in range(4)])
        total = jnp.sum(total, axis=1, keepdims=True)
        lanes8 = lax.broadcasted_iota(jnp.int32, (8, BLOCK), 1)
        return jnp.sum(jnp.where(lanes8 == cells8, total, 0.0), axis=0, keepdims=True)

    def near_state():
        none = [[nf[b * 3 + a] for b in range(lb)] for a in range(3)]
        return new_state(none, [nf[3 * lb + g] for g in range(lg)])

    def new_state(field, potential):
        mu = [
            [pol[b : b + 1] * (fixed[a : a + 1, lanes(b)] + field[a][b]) for b in range(lb)]
            for a in range(3)
        ]
        q = [base[g : g + 1] - resp[g : g + 1] * potential[g] for g in range(lg)]
        return mu, q

    scope = jax.named_scope
    with scope("barrier"):
        pl.semaphore_wait(barrier, greeted)
    signal(hello.at[0], beside, grp)
    for other in z_line:
        signal(hello.at[1], other, grp)
    with scope("send0"):
        share_sums(0)
        if DIRECT_P:
            share_direct(pos, prows, S_POS, S_PL, S_PR)
        else:
            share_group(pos, own * prows, prows, S_POS)
    for a in range(3):
        for b in range(lb):
            tgt[b * 3 + a] = jnp.transpose(
                jnp.broadcast_to(sites[a : a + 1, lanes(b)], (BLOCK, BLOCK))
            )
        for g in range(lg):
            tgt[(lb + g) * 3 + a] = jnp.transpose(
                jnp.broadcast_to(points[a : a + 1, lanes(g)], (BLOCK, BLOCK))
            )

    cells8 = lax.broadcasted_iota(jnp.int32, (8, BLOCK), 0)

    def far_rows(ref, j, c8):
        number = cells8 + c8 * 8
        dx = ref[0:1, lanes(j)] - (number.astype(F32) + 0.5)
        dy = ref[1:2, lanes(j)] - 0.5 + jnp.zeros_like(dx)
        dz = ref[2:3, lanes(j)] - 0.5 + jnp.zeros_like(dx)
        keep = jnp.abs(number - cell) >= 2
        s1, s3 = powers(dx, dy, dz)
        s3 = jnp.where(keep, s3, 0.0)
        return dx, dy, dz, s3, s3 * s1 * s1

    def far_build(c8, carry):
        row = pl.ds(pl.multiple_of(c8 * 8, 8), 8)
        low = pl.ds(pl.multiple_of(ncell + c8 * 8, 8), 8)
        answer = [jnp.zeros((8, BLOCK), F32) for _ in range(9)]
        for b in range(lb):
            dx, dy, dz, s3, s5 = far_rows(sites, b, c8)
            values = (*pair_tensor(dx, dy, dz, s3, s5), dx * s3, dy * s3, dz * s3)
            for n, v in enumerate(values):
                fd[b * 9 + n, row] = v
                answer[n] = answer[n] + v * pol[b : b + 1]
        charge = [[jnp.zeros((8, BLOCK), F32) for _ in range(3)] for _ in range(4)]
        for g in range(lg):
            dx, dy, dz, s3, s5 = far_rows(points, g, c8)
            for n, v in enumerate((dx, dy, dz)):
                fp[g * 3 + n, row] = v * s3
                change = v * s3 * resp[g : g + 1]
                charge[0][n] = charge[0][n] - change
                for a in range(3):
                    charge[1 + a][n] = charge[1 + a][n] - change * offsets(a, g)
        xx, xy, xz, yy, yz, zz, cx, cy, cz = answer
        halves = [(xx, xy), (xy, yy), (xz, yz), (xz, cx), (yz, cy), (zz, cz)]
        halves += [(c[0], c[1]) for c in charge]
        halves += [(c[2], jnp.zeros((8, BLOCK), F32)) for c in charge]
        for n, (top, bottom) in enumerate(halves):
            zst[n, row] = top
            zst[n, low] = bottom
        return carry

    with jax.named_scope("far_build"):
        lax.fori_loop(0, ncell // 8, far_build, 0)
        places = [
            [(a, a) for a in range(3)] + [(4 + a, a) for a in range(3)],
            [(a, 3 + a) for a in range(3)] + [(4 + a, 3 + a) for a in range(3)],
            [(3 + a, 6 + a) for a in range(4)],
            [(3 + a, 10 + a) for a in range(4)],
        ]
        flat = [jnp.sum(jnp.transpose(zst[n]), axis=0, keepdims=True) for n in range(14)]
        for t in range(4):
            value = jnp.zeros((8, BLOCK), F32)
            for at, n in places[t]:
                value = jnp.where(cells8 == at, flat[n], value)
            lin[grp, t] = value

    share_state(0)
    with scope("hello"):
        pl.semaphore_wait(hello.at[1], len(z_line))
        signal(hello.at[2], partner, grp)
        pl.semaphore_wait(hello.at[2], 1)
    def sent(ref, rows, sem_group, sem_left, sem_right):
        size = ngrp * rows
        drain(ref.at[pl.ds(0, (ngrp - 1) * rows)], send_sem.at[sem_group])

        @pl.when(cell < ncell - 1)
        def _():
            drain(ref.at[pl.ds(0, size)], send_sem.at[sem_right])

        @pl.when(cell > 0)
        def _():
            drain(ref.at[pl.ds(0, size)], send_sem.at[sem_left])

    def sent_all(k):
        if k == 0:
            sent(pos, prows, S_POS, S_PL, S_PR)
            drain(lin.at[pl.ds(0, ngrp - 1)], send_sem.at[S_LIN])
        drain(sa.at[pl.ds(0, ngrp - 1)], send_sem.at[S_SA + k])
        drain(tables[k].at[pl.ds(0, ncell - 1)], send_sem.at[S_TB + k])
        sent(windows[k], urows, S_W + k, S_FL + k, S_FR + k)

    def forward_window(k):
        (forward_partner if DIRECT_W[k] else forward)(
            windows[k], urows, S_W + k, S_FL + k, S_FR + k
        )

    answer = None
    for k in range(ITERS):
        with scope(f"share_cell#k={k}"):
            share_cell(k, answer)
        with scope(f"forward#k={k}"):
            if k == 0:
                (forward_partner if DIRECT_P else forward)(pos, prows, S_POS, S_PL, S_PR)
            if k > 0:
                forward_window(k)
                sent_all(k - 1)
        if k == 0:
            for d in ring_order(ngrp):
                copy_to(
                    lin.at[grp], lin.at[grp], send_sem.at[S_LIN], recv_sem.at[S_LIN],
                    (cell, group_at(d)),
                )
            with scope("wait_pos"):
                arrived(pos, prows, S_PL, S_PR)
            with scope("build"):
                build()
        with scope(f"own#k={k}"):
            apply_own(windows[k])
        with scope(f"wait_window#k={k}"):
            arrived(windows[k], urows, S_FL + k, S_FR + k)
        with scope(f"near#k={k}"):
            apply_near(windows[k])
        if k < ITERS - 1:
            with scope(f"sums#k={k + 1}"):
                put_sums(k + 1, *near_state())
                share_sums(k + 1)
        if k == 0:
            with scope("lin"):
                drain(lin.at[pl.ds(0, ngrp - 1)], recv_sem.at[S_LIN])
                for t in range(4):
                    lint[t] = functools.reduce(jnp.add, [lin[j, t] for j in range(ngrp)])
        with scope(f"wait_far#k={k}"):
            drain(tables[k].at[pl.ds(0, ncell - 1)], recv_sem.at[S_TB + k])
        with scope(f"far#k={k}"):
            mu, q = new_state(*apply_far(k))
        if k < ITERS - 1:
            with scope(f"send#k={k + 1}"):
                put_state(k + 1, mu, q)
                share_state(k + 1)
            with scope(f"answer#k={k + 1}"):
                answer = far_answer()
        else:
            for a in range(3):
                for b in range(lb):
                    out_mu[a : a + 1, lanes(b)] = mu[a][b]
            for g in range(lg):
                out_q[g : g + 1] = q[g]

    sent_all(ITERS - 1)


def body(
    ncell, ngrp,
    atom_sites, grid_points, dipole_guess, fixed_field, polarisability, base_charge, response,
    near_blocks, grid_blocks, source_blocks,
):
    lb, nb = near_blocks.shape
    nq = grid_blocks.shape[1]
    lg, nm = source_blocks.shape
    urows = 3 * lb + lg
    prows = 3 * lb + 3 * lg
    vmem = pl.BlockSpec(memory_space=pltpu.VMEM)
    tile = (BLOCK, BLOCK)
    window = pltpu.VMEM((3 * ngrp * urows, 1, BLOCK), F32)
    table = pltpu.VMEM((ncell, 1, BLOCK), F32)
    mu, q = pl.pallas_call(
        functools.partial(kernel, ncell, ngrp, lb, lg, nb, nq, nm),
        out_shape=(
            pltpu.VMEM((3, lb * BLOCK), F32),
            pltpu.VMEM((lg, BLOCK), F32),
        ),
        in_specs=[pl.BlockSpec(memory_space=pl.ANY)] * 10,
        out_specs=(vmem, vmem),
        scratch_shapes=[
            pltpu.SMEM(near_blocks.shape, jnp.int32),
            pltpu.SMEM(grid_blocks.shape, jnp.int32),
            pltpu.SMEM(source_blocks.shape, jnp.int32),
            pltpu.VMEM((3, lb * BLOCK), F32),
            pltpu.VMEM((3, lg * BLOCK), F32),
            pltpu.VMEM((3, lb * BLOCK), F32),
            pltpu.VMEM((3, lb * BLOCK), F32),
            pltpu.VMEM((lb, BLOCK), F32),
            pltpu.VMEM((lg, BLOCK), F32),
            pltpu.VMEM((lg, BLOCK), F32),
            pltpu.SMEM((lb * (nb + 1 + nq) + lg * nm,), jnp.int32),
            pltpu.SMEM((lb * (nb + 1 + nq) + lg * nm,), jnp.int32),
            window, window, window,
            pltpu.VMEM((3 * ngrp * prows, 1, BLOCK), F32),
            pltpu.VMEM((ITERS * ngrp, 1, BLOCK), F32),
            table, table, table,
            pltpu.VMEM(((lb + lg) * 3, *tile), F32),
            pltpu.VMEM((lb * (nb + 1) * 64, 8, BLOCK), F32),
            pltpu.VMEM((lb * nq * 48, 8, BLOCK), F32),
            pltpu.VMEM((lg * nm * 48, 8, BLOCK), F32),
            pltpu.VMEM((lb * 9, ncell, BLOCK), F32),
            pltpu.VMEM((lg * 3, ncell, BLOCK), F32),
            pltpu.VMEM((14, *tile), F32),
            pltpu.VMEM((ngrp, 4, 8, BLOCK), F32),
            pltpu.VMEM((4, 8, BLOCK), F32),
            pltpu.VMEM((ncell, BLOCK), F32),
            pltpu.VMEM((lg * nm * 3, 8, BLOCK), F32),
            pltpu.VMEM(((nb + 1) * 3 + nq, 8, BLOCK), F32),
            pltpu.VMEM((3 * lb + lg, *tile), F32),
            pltpu.VMEM((3 * lb + lg, 1, BLOCK), F32),
            pltpu.SemaphoreType.DMA((10,)),
            pltpu.SemaphoreType.DMA((19,)),
            pltpu.SemaphoreType.DMA((19,)),
            pltpu.SemaphoreType.REGULAR((3,)),
        ],
        compiler_params=pltpu.CompilerParams(
            collective_id=0, has_side_effects=True, vmem_limit_bytes=60 * 1024 * 1024
        ),
    )(
        near_blocks, grid_blocks, source_blocks,
        atom_sites, grid_points, dipole_guess, fixed_field,
        polarisability.reshape(lb, BLOCK), base_charge.reshape(lg, BLOCK),
        response.reshape(lg, BLOCK),
    )
    return mu, q.reshape(-1)


def solution(mesh):
    shared = P(None, ("cell", "grp"))
    flat = P(("cell", "grp"))
    rows = P(("cell", "grp"), None)
    return jax.shard_map(
        functools.partial(body, mesh.shape["cell"], mesh.shape["grp"]),
        mesh=mesh,
        in_specs=(shared, shared, shared, shared, flat, flat, flat, rows, rows, rows),
        out_specs=(shared, flat),
        check_vma=False,
    )
```
